512 devices in a mesh: dp: 64 (over z, y_lo, core), tensor: 8 (over x, y_hi).
Axes of the slice: x: 4, y: 4 (y_hi: 2, y_lo: 2; y = y_hi * 2 + y_lo), z: 16, core: 2. Of those that a mesh axis runs over, the one named last changes fastest.
Arguments:
- activations: bfloat16 [131072, 1024], P(('dp', 'tensor')), may hold values from -24 to 24
- gradients: bfloat16 [131072, 5472], P('dp', 'tensor'), may hold values from -6 to 6
- act_history: float32 [8, 16, 1024], P('tensor'), may hold values from 0.1 to 4
- grad_history: float32 [16, 5472], P(None, 'tensor'), may hold values from 0.1 to 4
- owner_rank: int32 [1024], replicated, may hold values from 0 to 7
- history_slot: int32 [6496], replicated, may hold values from 0 to 15
Outputs:
- weight_grad: float32 [1024, 5472], P('dp', 'tensor')
- act_history_out: float32 [8, 16, 1024], P('tensor')
- grad_history_out: float32 [16, 5472], P(None, 'tensor')
The draws below stay inside these ranges and needn't reach their ends.
All inputs are finite; a program needn't handle non-finite values.
Results may differ from the reference program's by a relative error of at most 0.0042.
Values may be sent and summed in bfloat16 or wider, within the bound.
A program may use at most 64 MiB of HBM per device.

```python
import math
import jax
import jax.numpy as jnp
from jax import lax

D = 1024
FF = 5472
HIST = 16
TOKENS = 131072
N_TENSOR = 8


def set_ends(values, own_key, least, high):
    longest = values.shape.index(max(values.shape))
    spots = []
    for shift in (0, 1):
        where = [jax.random.randint(jax.random.fold_in(own_key, axis), (), 0, length) for axis, length in enumerate(values.shape)]
        where[longest] = (where[longest] + shift) % values.shape[longest]
        spots.append(tuple(where))
    return values.at[spots[0]].set(least).at[spots[1]].set(high)


def with_spikes(values, own_key, source, target, shards_of, factor):
    owner, partner = [(jnp.arange(values.shape[dim]) // (values.shape[dim] // shards_of)).reshape([-1 if axis == dim else 1 for axis in range(values.ndim)]) for dim in (source, target)]
    chosen = jax.random.permutation(own_key, shards_of)[partner]
    strong = (owner == chosen) | (owner == (partner + shards_of // 2) % shards_of)
    return jnp.where(strong, factor * values, values)


def shard_levels(stream_key, shape, cuts, least, largest):
    def one(position, shards_of):
        draws = jax.random.uniform(jax.random.fold_in(jax.random.fold_in(stream_key, 6), position), (shards_of,), jnp.float32, least / len(cuts), largest / len(cuts))
        return jnp.repeat(jnp.exp(draws), shape[position] // shards_of).reshape((-1,) + (1,) * (len(shape) - position - 1))

    factor_of = one(*cuts[0])
    for cut in cuts[1:]:
        factor_of = factor_of * one(*cut)
    return factor_of


def gaussian(key, shape, width, limit, split=(), held_as=jnp.bfloat16):
    result = jax.random.normal(key, shape, jnp.float32) * width
    if len(split) > 0:
        result = shard_levels(key, shape, split, -0.22, 0.18) * result
    return jnp.clip(result, min=-limit, max=limit).astype(held_as)


def bell_draw_with(own_key, shape, deviation, most, split, heavy, held_as=jnp.bfloat16):
    result = deviation * jax.random.normal(own_key, shape, jnp.float32)
    if split:
        result = result * shard_levels(own_key, shape, split, -0.22, 0.18)
    return jnp.clip(with_spikes(result, jax.random.fold_in(own_key, 3), *heavy), -most, most).astype(held_as)


def setup_inputs(seed: int = 0) -> dict:
    splits = jax.random.split(jax.random.key(seed), 7)
    return {
        "activations": bell_draw_with(splits[0], (TOKENS, D), 1.0, 24.0, ((0, 512),), (0, 1, 512, 6.0)),
        "gradients": gaussian(splits[1], (TOKENS, FF), 1.0, 6.0, ((0, 64), (1, 8))),
        "act_history": jnp.clip(jnp.exp(math.log(4.0) - 3.6888794 * jax.random.uniform(splits[2], (N_TENSOR, HIST, D), jnp.float32) ** shard_levels(splits[2], (N_TENSOR, HIST, D), ((0, 8),), -0.2, 0.2)), 0.1, 4.0),
        "grad_history": jnp.clip(jnp.exp(math.log(4.0) - 3.6888794 * jax.random.uniform(splits[3], (HIST, FF), jnp.float32) ** shard_levels(splits[3], (HIST, FF), ((1, 8),), -0.2, 0.2)), 0.1, 4.0),
        "owner_rank": set_ends(jax.random.randint(splits[4], (D,), 0, N_TENSOR), jax.random.fold_in(splits[4], 1), 0, N_TENSOR - 1).astype(jnp.int32),
        "history_slot": set_ends(jax.random.randint(splits[5], (D + FF,), 0, HIST), jax.random.fold_in(splits[5], 1), 0, HIST - 1).astype(jnp.int32),
    }


QUANT_LIMIT = 448.0
SCALE_FLOOR = 0.25

def quantize(values, scale):
    scaled = values.astype(jnp.float32) * scale
    return jnp.clip(scaled, -QUANT_LIMIT, QUANT_LIMIT).astype(jnp.bfloat16)

def place_peaks(history, peaks, slots):
    rows = lax.broadcasted_iota(jnp.int32, history.shape, 0)
    return jnp.where(rows == slots.astype(jnp.int32)[None, :], peaks[None, :], history)

def reference(activations, gradients, act_history, grad_history, owner_rank, history_slot):
    ranks = lax.broadcasted_iota(jnp.int32, act_history.shape, 0)
    picked = jnp.where(ranks == owner_rank.astype(jnp.int32)[None, None, :], act_history, jnp.float32(0.0))
    current_history = lax.optimization_barrier(jnp.sum(picked, axis=0))
    act_scale = QUANT_LIMIT / jnp.maximum(lax.optimization_barrier(jnp.max(current_history, axis=0)), SCALE_FLOOR)
    grad_scale = QUANT_LIMIT / jnp.maximum(lax.optimization_barrier(jnp.max(grad_history, axis=0)), SCALE_FLOOR)
    act_quant = quantize(activations, act_scale)
    block_width = FF // 4
    results = []
    for block_index in range(4):
        first_col = block_index * block_width
        grad_block = quantize(gradients[:, first_col:first_col + block_width], grad_scale[first_col:first_col + block_width])
        results.append(jnp.dot(act_quant.T, grad_block, preferred_element_type=jnp.float32))
    summed = jnp.concatenate(results, axis=1)
    grad_factor = 1.0 / math.sqrt(TOKENS)
    weight_grad = summed / (act_scale[:, None] * grad_scale[None, :]) * grad_factor
    act_peak = lax.optimization_barrier(jnp.max(jnp.abs(activations), axis=0)).astype(jnp.float32)
    grad_peak = lax.optimization_barrier(jnp.max(jnp.abs(gradients), axis=0)).astype(jnp.float32)
    updated = place_peaks(current_history, act_peak, history_slot[:D])
    act_history_out = jnp.broadcast_to(updated[None], (N_TENSOR, HIST, D))
    grad_history_out = place_peaks(grad_history, grad_peak, history_slot[D:])
    return (weight_grad, act_history_out, grad_history_out)
```

```python
import functools
import math

import jax
import jax.numpy as jnp
from jax import lax
from jax.experimental import pallas as pl
from jax.experimental.pallas import tpu as pltpu
from jax.sharding import PartitionSpec as P

QUANT_LIMIT = 448.0
SCALE_FLOOR = 0.25
LANES = 128
MESH = pl.DeviceIdType.MESH


def kernel(
    nz, nx, acts, grads, ahist, ghist, owner,
    sum_out, hist_out, peak_out, gpeak_out, ascale_out, gscale_out,
    g, acol, graw, gq, q, scales, mh, msg, hr, hb, ch, pv, pcore, pylo, pz1, pz2,
    part, s1, r1, s2, r2, keep2, s3, rb,
    ld_g, ld_a, ld_r,
    sy, ry, sxo, rxo, sxp, rxp, sf, rf,
    sm, rm, sh1, rh1, sh3, rh3, sh4, rh4,
    sp2, rp2, sp3, rp3, sp4, rp4, sp5, rp5,
    sr1, rr1, sr2, rr2, sr3, rr3,
):
    nc = nz // 2
    nt = 2 * nx
    rows = acts.shape[0]
    width = grads.shape[1]
    pb = 4
    t = lax.axis_index("tensor")
    dpi = lax.axis_index("dp")
    x, yh = t // 2, t % 2
    z, yl, c = dpi // 4, (dpi // 2) % 2, dpi % 2
    q_slot = 2 * x + (1 - yh)
    xr, xl = (x + 1) % nx, (x + nx - 1) % nx

    def tensor_dev(tt):
        return {"dp": dpi, "tensor": tt}

    def dp_dev(zz, yy, cc):
        return {"dp": zz * 4 + yy * 2 + cc, "tensor": t}

    def rcopy(src, dst, ss, rs, device):
        return pltpu.make_async_remote_copy(
            src_ref=src, dst_ref=dst, send_sem=ss, recv_sem=rs,
            device_id=device, device_id_type=MESH,
        )

    def chunk(s):
        half = (s + 1) // 2
        return (z // 2 + nc // 2 + (1 - 2 * (s % 2)) * half + 2 * nc) % nc

    partner_y = tensor_dev(q_slot)
    right = tensor_dev(2 * xr + yh)
    left = tensor_dev(2 * xl + yh)
    other_core = dp_dev(z, yl, 1 - c)
    other_yl = dp_dev(z, 1 - yl, c)

    def load_g(s):
        col = pl.multiple_of(chunk(s) * LANES, LANES)
        return pltpu.make_async_copy(acts.at[:, pl.ds(col, LANES)], g.at[s, t], ld_g.at[s])

    for s in range(nc):
        load_g(s).start()
    load_a = pltpu.make_async_copy(acts, acol, ld_a)
    load_a.start()
    load_r = pltpu.make_async_copy(grads, graw, ld_r)
    load_r.start()

    bar = pltpu.get_barrier_semaphore()
    for i in range(1, nt):
        pl.semaphore_signal(bar, inc=1, device_id=tensor_dev((t + i) % nt), device_id_type=MESH)
    pl.semaphore_signal(bar, inc=1, device_id=other_core, device_id_type=MESH)
    pl.semaphore_signal(bar, inc=1, device_id=other_yl, device_id_type=MESH)
    for i in range(1, nz):
        pl.semaphore_signal(bar, inc=1, device_id=dp_dev((z + i) % nz, yl, c), device_id_type=MESH)

    held = jnp.where(owner[...] == t, ahist[0], jnp.float32(0.0))
    mh[...] = held
    msg[t, :, : nc * LANES] = jnp.max(held, axis=0, keepdims=True)
    hcol = pl.multiple_of((z % nc) * LANES, LANES)
    hrow = pl.multiple_of(c * 8, 8)
    hr[t] = mh[pl.ds(hrow, 8), pl.ds(hcol, LANES)]
    gscale = QUANT_LIMIT / jnp.maximum(jnp.max(ghist[...], axis=0, keepdims=True), SCALE_FLOOR)
    gscale_out[...] = gscale

    pl.semaphore_wait(bar, nt - 1 + 2 + nz - 1)

    def y_copy(s):
        return rcopy(g.at[s, t], g.at[s, t], sy.at[s], ry.at[s], partner_y)

    def y_arrival(s):
        return rcopy(g.at[s, q_slot], g.at[s, q_slot], sy.at[s], ry.at[s], partner_y)

    def xo_copy(s, d):
        return rcopy(g.at[s, t], g.at[s, t], sxo.at[s, d], rxo.at[s, d], right if d == 0 else left)

    def xp_copy(s, d):
        return rcopy(
            g.at[s, q_slot], g.at[s, q_slot], sxp.at[s, d], rxp.at[s, d], right if d == 0 else left
        )

    lo, lp = 2 * xl + yh, 2 * xl + 1 - yh
    ro, rp = 2 * xr + yh, 2 * xr + 1 - yh

    def xo_arrival(s, d):
        slot = lo if d == 0 else ro
        return rcopy(g.at[s, slot], g.at[s, slot], sxo.at[s, d], rxo.at[s, d], right)

    def xp_arrival(s, d):
        slot = lp if d == 0 else rp
        return rcopy(g.at[s, slot], g.at[s, slot], sxp.at[s, d], rxp.at[s, d], right)

    def f_copy(s, d):
        if d == 0:
            return rcopy(g.at[s, lo], g.at[s, lo], sf.at[s, 0], rf.at[s, 0], right)
        return rcopy(g.at[s, rp], g.at[s, rp], sf.at[s, 1], rf.at[s, 1], left)

    xf = (x + 2) % nx

    def f_arrival(s, d):
        slot = 2 * xf + yh if d == 0 else 2 * xf + 1 - yh
        return rcopy(g.at[s, slot], g.at[s, slot], sf.at[s, d], rf.at[s, d], right)

    def stage_own(s):
        y_copy(s).start()
        xo_copy(s, 0).start()
        xo_copy(s, 1).start()

    def stage_partner(s):
        y_arrival(s).wait_recv()
        xp_copy(s, 0).start()
        xp_copy(s, 1).start()

    def stage_far(s):
        xo_arrival(s, 0).wait_recv()
        f_copy(s, 0).start()
        xp_arrival(s, 1).wait_recv()
        f_copy(s, 1).start()

    def stage_finish(s):
        xo_arrival(s, 1).wait_recv()
        xp_arrival(s, 0).wait_recv()
        f_arrival(s, 0).wait_recv()
        f_arrival(s, 1).wait_recv()

    for s in range(nc):
        load_g(s).wait()
        if s < 3:
            stage_own(s)

    def m_copy(i):
        return rcopy(msg.at[t], msg.at[t], sm.at[i], rm.at[i], tensor_dev((t + i) % nt))

    def h1_copy(i):
        return rcopy(hr.at[t], hr.at[t], sh1.at[i], rh1.at[i], tensor_dev((t + i) % nt))

    load_a.wait()
    msg[t, :, nc * LANES :] = jnp.max(jnp.abs(acol[...].astype(jnp.float32)), axis=0, keepdims=True)
    for i in range(1, nt):
        m_copy(i).start()
    for i in range(1, nt):
        h1_copy(i).start()

    load_r.wait()
    block = 64

    def quant_grads(i, carry):
        at = pl.ds(pl.multiple_of(i * block, block), block)
        v = graw[at, :].astype(jnp.float32)
        gq[at, :] = jnp.clip(v * gscale, -QUANT_LIMIT, QUANT_LIMIT).astype(jnp.bfloat16)
        return jnp.maximum(carry, jnp.max(jnp.abs(v).reshape(block // 8, 8, width), axis=0))

    blocks = graw.shape[0] // block
    gpeak8 = lax.fori_loop(0, blocks // 2, quant_grads, jnp.zeros((8, width), jnp.float32))
    stage_partner(0)
    gpeak8 = lax.fori_loop(blocks // 2, blocks, quant_grads, gpeak8)
    gpeak = jnp.max(gpeak8, axis=0, keepdims=True)

    if nc > 1:
        stage_partner(1)
    stage_far(0)

    for i in range(1, nt):
        frm = (t + nt - i) % nt
        rcopy(msg.at[frm], msg.at[frm], sm.at[i], rm.at[i], partner_y).wait_recv()
    hmax = msg[0, :, : nc * LANES]
    apeak = msg[0, :, nc * LANES :]
    for i in range(1, nt):
        hmax = hmax + msg[i, :, : nc * LANES]
        apeak = jnp.maximum(apeak, msg[i, :, nc * LANES :])
    ascale = QUANT_LIMIT / jnp.maximum(hmax, SCALE_FLOOR)
    ascale_out[...] = ascale
    for k in range(nc):
        scales[k] = ascale[:, k * LANES : (k + 1) * LANES]
    ca = nc * LANES
    pv[:, :] = jnp.zeros(pv.shape, jnp.float32)
    pv[:, :ca] = apeak
    pv[:, ca : ca + width] = gpeak

    def r1_copy(s):
        return rcopy(s1.at[s], r1.at[s], sr1.at[s], rr1.at[s], other_core)

    def r2_copy(s):
        return rcopy(s2.at[s], r2.at[s], sr2.at[s], rr2.at[s], other_yl)

    def r3_copy(s, zo, zz):
        return rcopy(s3.at[s, zo], rb.at[z], sr3.at[s, zo], rr3.at[z], dp_dev(zz, yl, c))

    def compute(s):
        scale = scales[chunk(s)]
        for i in range(nt):
            v = g[s, i].astype(jnp.float32) * scale
            q[pl.ds(i * rows, rows), :] = jnp.clip(v, -QUANT_LIMIT, QUANT_LIMIT).astype(jnp.bfloat16)
        out = lax.dot_general(
            q[...], gq[...], (((0,), (0,)), ((), ())), preferred_element_type=jnp.float32
        )
        part[...] = out.reshape(8, 16, width)
        for i in range(4):
            s1[s, i] = part[2 * i + 1 - c].astype(jnp.bfloat16)

    def finish_r1(s):
        r1_copy(s).wait_recv()
        for zo in range(2):
            a = 2 * zo + 1 - yl
            b = 2 * zo + yl
            s2[s, zo] = (part[2 * a + c] + r1[s, a].astype(jnp.float32)).astype(jnp.bfloat16)
            keep2[zo] = part[2 * b + c] + r1[s, b].astype(jnp.float32)
        r2_copy(s).start()

    def finish_r2(s):
        r2_copy(s).wait_recv()
        k = chunk(s)
        for zo in range(2):
            s3[s, zo] = (keep2[zo] + r2[s, zo].astype(jnp.float32)).astype(jnp.bfloat16)
        for zo in range(2):
            zz = 2 * k + zo

            @pl.when(zz == z)
            def _():
                rb[z] = s3[s, zo]

            @pl.when(zz != z)
            def _():
                r3_copy(s, zo, zz).start()

    def p2_copy():
        return rcopy(pv, pcore, sp2, rp2, other_core)

    def p3_copy():
        return rcopy(pcore, pylo, sp3, rp3, other_yl)

    za, zb = z // pb, z % pb

    def p4_copy(i):
        return rcopy(
            pylo, pz1.at[i], sp4.at[i], rp4.at[i], dp_dev(za * pb + (zb + i) % pb, yl, c)
        )

    na = nz // pb

    def p5_copy(i):
        return rcopy(
            pz1.at[0], pz2.at[i], sp5.at[i], rp5.at[i], dp_dev(((za + i) % na) * pb + zb, yl, c)
        )

    def h3_copy(i):
        dst = ch.at[pl.ds(hrow, 8), pl.ds(hcol, LANES)]
        zz = (z // nc) * nc + (z % nc + i) % nc
        return rcopy(hb, dst, sh3.at[i], rh3.at[i], dp_dev(zz, yl, c))

    def h3_arrival(i):
        col = pl.multiple_of(((z % nc + nc - i) % nc) * LANES, LANES)
        dst = ch.at[pl.ds(hrow, 8), pl.ds(col, LANES)]
        return rcopy(hb, dst, sh3.at[i], rh3.at[i], other_core)

    def h4_copy():
        half = ch.at[pl.ds(hrow, 8), :]
        return rcopy(half, half, sh4, rh4, other_core)

    def h4_arrival():
        half = ch.at[pl.ds(pl.multiple_of(8 - hrow, 8), 8), :]
        return rcopy(half, half, sh4, rh4, other_core)

    def side_work(s):
        def h2():
            for i in range(1, nt):
                frm = (t + nt - i) % nt
                rcopy(hr.at[frm], hr.at[frm], sh1.at[i], rh1.at[i], partner_y).wait_recv()
            total = hr[0]
            for i in range(1, nt):
                total = total + hr[i]
            hb[...] = total
            ch[pl.ds(hrow, 8), pl.ds(hcol, LANES)] = total
            for i in range(1, nc):
                h3_copy(i).start()

        def p3():
            p2_copy().wait_recv()
            pcore[...] = jnp.maximum(pcore[...], pv[...])
            p3_copy().start()

        def p4():
            p3_copy().wait_recv()
            pylo[...] = jnp.maximum(pylo[...], pcore[...])
            for i in range(1, pb):
                p4_copy(i).start()

        def p5():
            m = pylo[...]
            for i in range(1, pb):
                p4_copy(i).wait_recv()
                m = jnp.maximum(m, pz1[i])
            pz1[0] = m
            for i in range(1, na):
                p5_copy(i).start()

        def p6():
            m = pz1[0]
            for i in range(1, na):
                p5_copy(i).wait_recv()
                m = jnp.maximum(m, pz2[i])
            peak_out[...] = m[:, :ca]
            gpeak_out[...] = m[:, ca : ca + width]

        def h4():
            for i in range(1, nc):
                h3_arrival(i).wait_recv()
            h4_copy().start()

        def h5():
            h4_arrival().wait_recv()
            hist_out[...] = ch[...]

        todo = [[p2_copy().start], [h2], [p3], [p4], [p5], [h4], [p6, h5]]
        for at, works in enumerate(todo):
            for work in works:
                pl.when(s == min(at, nc - 1))(work)

    def step(s, carry):
        @pl.when(s + 3 < nc)
        def _():
            stage_own(s + 3)

        @pl.when(s >= 1)
        def _():
            finish_r1(s - 1)

        @pl.when(s + 2 < nc)
        def _():
            stage_partner(s + 2)

        @pl.when(s + 1 < nc)
        def _():
            stage_far(s + 1)

        stage_finish(s)
        compute_into(s)
        r1_copy(s).start()

        @pl.when(s >= 1)
        def _():
            finish_r2(s - 1)

        side_work(s)
        return carry

    def compute_into(s):
        compute(s)

    lax.fori_loop(0, nc, step, 0)
    last = nc - 1
    finish_r1(last)
    finish_r2(last)

    total = rb[z].astype(jnp.float32)
    for i in range(1, nz):
        frm = (z + i) % nz
        rcopy(rb.at[frm], rb.at[frm], sr1.at[0], rr3.at[frm], other_core).wait_recv()
        total = total + rb[frm].astype(jnp.float32)
    sum_out[...] = total

    def drain(s, carry):
        y_copy(s).wait_send()
        for d in range(2):
            xo_copy(s, d).wait_send()
            xp_copy(s, d).wait_send()
            f_copy(s, d).wait_send()
        r1_copy(s).wait_send()
        r2_copy(s).wait_send()
        k = chunk(s)
        for zo in range(2):
            @pl.when(2 * k + zo != z)
            def _():
                r3_copy(s, zo, z).wait_send()
        return carry

    lax.fori_loop(0, nc, drain, 0)
    for i in range(1, nt):
        m_copy(i).wait_send()
        h1_copy(i).wait_send()
    for i in range(1, nc):
        h3_copy(i).wait_send()
    h4_copy().wait_send()
    p2_copy().wait_send()
    p3_copy().wait_send()
    for i in range(1, pb):
        p4_copy(i).wait_send()
    for i in range(1, na):
        p5_copy(i).wait_send()


def fused(acts, grads, ahist, ghist, owner, nz, nx):
    rows, model = acts.shape
    tokens, width = grads.shape
    nc, nt = nz // 2, 2 * nx
    na, pb = nz // 4, 4
    pw = model + -(-width // LANES) * LANES
    f32, bf16 = jnp.float32, jnp.bfloat16
    dma = pltpu.SemaphoreType.DMA
    vm = pltpu.VMEM
    scratch = [
        vm((nc, nt, rows, LANES), bf16),
        vm((rows, model), bf16),
        vm((tokens, width), bf16),
        vm((tokens, width), bf16),
        vm((tokens, LANES), bf16),
        vm((nc, 1, LANES), f32),
        vm((16, model), f32),
        vm((nt, 1, 2 * model), f32),
        vm((nt, 8, LANES), f32),
        vm((8, LANES), f32),
        vm((16, model), f32),
        vm((1, pw), f32),
        vm((1, pw), f32),
        vm((1, pw), f32),
        vm((pb, 1, pw), f32),
        vm((max(na, 2), 1, pw), f32),
        vm((8, 16, width), f32),
        vm((nc, 4, 16, width), bf16),
        vm((nc, 4, 16, width), bf16),
        vm((nc, 2, 16, width), bf16),
        vm((nc, 2, 16, width), bf16),
        vm((2, 16, width), f32),
        vm((nc, 2, 16, width), bf16),
        vm((nz, 16, width), bf16),
        dma((nc,)), dma, dma,
        dma((nc,)), dma((nc,)),
        dma((nc, 2)), dma((nc, 2)), dma((nc, 2)), dma((nc, 2)), dma((nc, 2)), dma((nc, 2)),
        dma((nt,)), dma((nt,)), dma((nt,)), dma((nt,)), dma((nc,)), dma((nc,)), dma, dma,
        dma, dma, dma, dma, dma((pb,)), dma((pb,)), dma((max(na, 2),)), dma((max(na, 2),)),
        dma((nc,)), dma((nc,)), dma((nc,)), dma((nc,)), dma((nc, 2)), dma((nz,)),
    ]
    vspec = pl.BlockSpec(memory_space=pltpu.VMEM)
    anyspec = pl.BlockSpec(memory_space=pl.ANY)
    return pl.pallas_call(
        functools.partial(kernel, nz, nx),
        out_shape=[
            jax.ShapeDtypeStruct((16, width), f32),
            jax.ShapeDtypeStruct((16, model), f32),
            jax.ShapeDtypeStruct((1, model), f32),
            jax.ShapeDtypeStruct((1, width), f32),
            jax.ShapeDtypeStruct((1, model), f32),
            jax.ShapeDtypeStruct((1, width), f32),
        ],
        in_specs=[anyspec, anyspec, vspec, vspec, vspec],
        out_specs=[vspec] * 6,
        scratch_shapes=scratch,
        compiler_params=pltpu.CompilerParams(
            collective_id=0, has_side_effects=True, vmem_limit_bytes=48 * 1024 * 1024
        ),
    )(acts, grads, ahist, ghist, owner)


def body(nz, nx, activations, gradients, act_history, grad_history, owner_rank, history_slot):
    model = act_history.shape[2]
    width = gradients.shape[1]
    my_rank = lax.axis_index("tensor")
    summed, current, act_peak, grad_peak, act_scale, grad_scale = fused(
        activations, gradients, act_history, grad_history, owner_rank.reshape(1, model), nz, nx
    )
    grad_factor = 1.0 / math.sqrt(gradients.shape[0] * lax.axis_size("dp"))
    row_base = lax.axis_index("dp") * 16
    row_scale = lax.dynamic_slice(act_scale, (0, row_base), (1, 16)).reshape(16, 1)
    weight_grad = summed / (row_scale * grad_scale) * grad_factor
    act_slots = history_slot[:model]
    grad_slots = lax.dynamic_slice_in_dim(history_slot, model + my_rank * width, width, 0)

    def place(history, peaks, slots):
        at = lax.broadcasted_iota(jnp.int32, history.shape, 0)
        return jnp.where(at == slots[None, :], peaks, history)

    act_history_out = place(current, act_peak, act_slots)[None]
    grad_history_out = place(grad_history, grad_peak, grad_slots)
    return (weight_grad, act_history_out, grad_history_out)


def solution(mesh):
    nz = mesh.shape["dp"] // 4
    nx = mesh.shape["tensor"] // 2
    placed = (
        P(("dp", "tensor"), None),
        P("dp", "tensor"),
        P("tensor", None, None),
        P(None, "tensor"),
        P(),
        P(),
    )
    return jax.shard_map(
        functools.partial(body, nz, nx),
        mesh=mesh,
        in_specs=placed,
        out_specs=(P("dp", "tensor"), P("tensor", None, None), P(None, "tensor")),
        check_vma=False,
    )
```

```python
import functools
import math

import jax
import jax.numpy as jnp
from jax import lax
from jax.experimental import pallas as pl
from jax.experimental.pallas import tpu as pltpu
from jax.sharding import PartitionSpec as P

QUANT_LIMIT = 448.0
SCALE_FLOOR = 0.25
LANES = 128
BLOCK = 64
MESH = pl.DeviceIdType.MESH


def kernel(
    nz, nx, acts, grads, ahist, ghist, owner,
    sum_out, hist_out, peak_out, gpeak_out, ascale_out, gscale_out,
    g, acol, graw, gq, q, ah, gh, ow, gcol, gpk, scales, mh, small, hb, ch,
    pv, pcore, pylo, pzz, pfar,
    part, s1, r1, s2, r2, keep2, s3, r3, keep3, s4, rb, own_sum,
    ld_g, ld_x,
    sy, ry, sxo, rxo, sxp, rxp, sf, rf, sy2, ry2,
    sh3, rh3, sh4, rh4, sp2, rp2, sp3, rp3, sp4, rp4, sp5, rp5,
    sr1, rr1, sr2, rr2, sr3, rr3, sr4, rr4, tok1, tok2,
):
    nc = nz // 2
    nt = 2 * nx
    early = max(3 * nc // 8, 1)
    tok_step = min(3, nc - 1)
    rows = acts.shape[0]
    width, tokens = grads.shape
    wp = gq.shape[0]
    t = lax.axis_index("tensor")
    dpi = lax.axis_index("dp")
    x, yh = t // 2, t % 2
    z, yl, c = dpi // 4, (dpi // 2) % 2, dpi % 2
    zp, zq = z // 2, z % 2
    xr, xl, xf = (x + 1) % nx, (x + nx - 1) % nx, (x + 2) % nx
    yo = 1 - yh

    def tensor_dev(tt):
        return {"dp": dpi, "tensor": tt}

    def dp_dev(zz, yy, cc):
        return {"dp": zz * 4 + yy * 2 + cc, "tensor": t}

    def pair_dev(pp):
        return dp_dev(2 * pp + zq, yl, c)

    def rcopy(src, dst, ss, rs, device):
        return pltpu.make_async_remote_copy(
            src_ref=src, dst_ref=dst, send_sem=ss, recv_sem=rs,
            device_id=device, device_id_type=MESH,
        )

    def signal(sem, device):
        pl.semaphore_signal(sem, inc=1, device_id=device, device_id_type=MESH)

    def chunk(s):
        half = (s + 1) // 2
        return (zp + nc // 2 + (1 - 2 * (s % 2)) * half + 2 * nc) % nc

    partner_y = tensor_dev(2 * x + yo)
    right = tensor_dev(2 * xr + yh)
    left = tensor_dev(2 * xl + yh)
    other_core = dp_dev(z, yl, 1 - c)
    other_yl = dp_dev(z, 1 - yl, c)
    other_z = dp_dev(2 * zp + 1 - zq, yl, c)

    def load_g(s):
        col = pl.multiple_of(chunk(s) * LANES, LANES)
        return pltpu.make_async_copy(acts.at[:, pl.ds(col, LANES)], g.at[s, t], ld_g.at[s])

    loads = [
        pltpu.make_async_copy(src, dst, ld_x.at[i])
        for i, (src, dst) in enumerate(
            [(ahist, ah), (owner, ow), (ghist, gh), (acts, acol), (grads, graw)]
        )
    ]
    loads[0].start()
    loads[1].start()
    for s in range(nc):
        load_g(s).start()
    for i in (3, 2, 4):
        loads[i].start()

    bar = pltpu.get_barrier_semaphore()
    for device in (partner_y, right, left, other_core, other_yl, other_z):
        signal(bar, device)
    for i in range(1, nc):
        @pl.when(jnp.logical_and(zp < early, zp + i < nc))
        def _():
            signal(bar, pair_dev(zp + i))

    def to_rows(vec, at, count):
        for k in range(count):
            small[t, at + k : at + k + 1, :] = vec[:, k * LANES : (k + 1) * LANES]

    loads[0].wait()
    loads[1].wait()
    held = jnp.where(ow[...] == t, ah[0], jnp.float32(0.0))
    mh[...] = held
    to_rows(jnp.max(held, axis=0, keepdims=True), 0, nc)
    hcol = pl.multiple_of(zp * LANES, LANES)
    hrow = pl.multiple_of(c * 8, 8)
    small[t, 8:16, :] = mh[pl.ds(hrow, 8), pl.ds(hcol, LANES)]
    loads[3].wait()
    to_rows(jnp.max(jnp.abs(acol[...].astype(jnp.float32)), axis=0, keepdims=True), 16, nc)

    pl.semaphore_wait(bar, 6 + jnp.minimum(zp, early))
    for i in range(early):
        @pl.when(i < zp)
        def _():
            signal(tok1, pair_dev(i))

    def at_slot(s, xx, yy):
        if isinstance(s, int) and s == nc:
            return small.at[2 * xx + yy]
        return g.at[s, 2 * xx + yy]

    def y_copy(s):
        return rcopy(at_slot(s, x, yh), at_slot(s, x, yh), sy.at[s], ry.at[s], partner_y)

    def y_arrival(s):
        return rcopy(at_slot(s, x, yo), at_slot(s, x, yo), sy.at[s], ry.at[s], partner_y)

    def xo_copy(s, d):
        a = at_slot(s, x, yh)
        return rcopy(a, a, sxo.at[s, d], rxo.at[s, d], right if d == 0 else left)

    def xo_arrival(s, d):
        a = at_slot(s, xl if d == 0 else xr, yh)
        return rcopy(a, a, sxo.at[s, d], rxo.at[s, d], right)

    def xp_copy(s, d):
        a = at_slot(s, x, yo)
        return rcopy(a, a, sxp.at[s, d], rxp.at[s, d], right if d == 0 else left)

    def xp_arrival(s, d):
        a = at_slot(s, xl if d == 0 else xr, yo)
        return rcopy(a, a, sxp.at[s, d], rxp.at[s, d], right)

    def far_own(s, d):
        a = at_slot(s, xl if d == 0 else xr, yh)
        return rcopy(a, a, sf.at[s, 0], rf.at[s, 0], right if d == 0 else left)

    def far_own_arrival(s):
        a = at_slot(s, xf, yh)
        return rcopy(a, a, sf.at[s, 0], rf.at[s, 0], right)

    def far_other(s, d):
        a = at_slot(s, xl if d == 0 else xr, yo)
        return rcopy(a, a, sf.at[s, 1], rf.at[s, 1], right if d == 0 else left)

    def far_other_arrival(s):
        a = at_slot(s, xf, yo)
        return rcopy(a, a, sf.at[s, 1], rf.at[s, 1], right)

    def y2_copy(s):
        a = at_slot(s, xf, yh)
        return rcopy(a, a, sy2.at[s], ry2.at[s], partner_y)

    def y2_arrival(s):
        a = at_slot(s, xf, yo)
        return rcopy(a, a, sy2.at[s], ry2.at[s], partner_y)

    def cond(pred, work):
        if isinstance(pred, bool):
            if pred:
                work()
        else:
            pl.when(pred)(work)

    def kind_a(s):
        if isinstance(s, int) and s == nc:
            return True
        return s % 7 == 0

    def kind_c(s):
        if isinstance(s, int) and s == nc:
            return False
        return s % 7 != 0

    def stage_own(s):
        y_copy(s).start()
        xo_copy(s, 0).start()
        xo_copy(s, 1).start()

    def stage_partner(s):
        y_arrival(s).wait_recv()
        xp_copy(s, 0).start()
        xp_copy(s, 1).start()

    def stage_far_own(s):
        def go(d):
            xo_arrival(s, d).wait_recv()
            far_own(s, d).start()

        cond(s % 2 == 0, lambda: go(0))
        cond(s % 2 == 1, lambda: go(1))

    def stage_far_other(s):
        def kind_a_work():
            def go(d):
                xp_arrival(s, d).wait_recv()
                far_other(s, d).start()

            cond(s % 2 == 0, lambda: go(1))
            cond(s % 2 == 1, lambda: go(0))

        def kind_c_work():
            far_own_arrival(s).wait_recv()
            y2_copy(s).start()

        cond(kind_a(s), kind_a_work)
        cond(kind_c(s), kind_c_work)

    def stage_finish(s):
        def even():
            xo_arrival(s, 1).wait_recv()

        def odd():
            xo_arrival(s, 0).wait_recv()

        cond(s % 2 == 0, even)
        cond(s % 2 == 1, odd)

        def kind_a_work():
            cond(s % 2 == 0, lambda: xp_arrival(s, 0).wait_recv())
            cond(s % 2 == 1, lambda: xp_arrival(s, 1).wait_recv())
            far_own_arrival(s).wait_recv()
            far_other_arrival(s).wait_recv()

        def kind_c_work():
            xp_arrival(s, 0).wait_recv()
            xp_arrival(s, 1).wait_recv()
            y2_arrival(s).wait_recv()

        cond(kind_a(s), kind_a_work)
        cond(kind_c(s), kind_c_work)

    stage_own(nc)
    for s in range(nc):
        load_g(s).wait()
        if s < 3:
            stage_own(s)

    loads[2].wait()
    gscale = QUANT_LIMIT / jnp.maximum(jnp.max(gh[...], axis=0, keepdims=True), SCALE_FLOOR)
    gscale_out[...] = gscale
    pad = jnp.zeros((1, wp - width), jnp.float32)
    gcol[...] = jnp.broadcast_to(jnp.concatenate([gscale, pad], axis=1), (LANES, wp)).T
    loads[4].wait()

    def quant_rows(at, count):
        scale = gcol[at, :]
        top = jnp.zeros((count, LANES), jnp.float32)
        for j in range(tokens // LANES):
            v = graw[at, j * LANES : (j + 1) * LANES].astype(jnp.float32)
            gq[at, j * LANES : (j + 1) * LANES] = jnp.clip(
                v * scale, -QUANT_LIMIT, QUANT_LIMIT
            ).astype(jnp.bfloat16)
            top = jnp.maximum(top, jnp.abs(v))
        gpk[at, :] = top

    def quant_block(i, carry):
        quant_rows(pl.ds(pl.multiple_of(i * BLOCK, BLOCK), BLOCK), BLOCK)
        return carry

    full = width // BLOCK
    lax.fori_loop(0, full // 3, quant_block, 0)
    stage_partner(nc)
    stage_partner(0)
    stage_far_own(nc)
    stage_far_own(0)
    lax.fori_loop(full // 3, 2 * full // 3, quant_block, 0)
    if nc > 1:
        stage_partner(1)
        stage_far_own(1)
    stage_far_other(nc)
    stage_far_other(0)
    lax.fori_loop(2 * full // 3, full, quant_block, 0)
    if width > full * BLOCK:
        quant_rows(slice(full * BLOCK, width), width - full * BLOCK)
    gq[width:, :] = jnp.zeros((wp - width, tokens), jnp.bfloat16)
    gpk[width:, :] = jnp.zeros((wp - width, LANES), jnp.float32)
    gpeak = jnp.max(gpk[...].T, axis=0, keepdims=True)

    stage_finish(nc)
    total_small = small[0]
    apeak = small[0, 16:24, :]
    for i in range(1, nt):
        total_small = total_small + small[i]
        apeak = jnp.maximum(apeak, small[i, 16:24, :])
    ascale = QUANT_LIMIT / jnp.maximum(total_small[0:8, :], SCALE_FLOOR)
    for k in range(nc):
        scales[k] = ascale[k : k + 1, :]
        ascale_out[:, k * LANES : (k + 1) * LANES] = ascale[k : k + 1, :]
    hb[...] = total_small[8:16, :]
    ch[pl.ds(hrow, 8), pl.ds(hcol, LANES)] = total_small[8:16, :]
    pv[0:8, :] = apeak
    for k in range(wp // LANES):
        pv[8 + k : 9 + k, :] = gpeak[:, k * LANES : (k + 1) * LANES]
    pv[8 + wp // LANES :, :] = jnp.zeros((8 - wp // LANES, LANES), jnp.float32)

    def r1_copy(s):
        return rcopy(s1.at[s], r1.at[s], sr1.at[s], rr1.at[s], other_core)

    def r2_copy(s):
        return rcopy(s2.at[s], r2.at[s], sr2.at[s], rr2.at[s], other_yl)

    def r3_copy(s):
        return rcopy(s3.at[s], r3.at[s], sr3.at[s], rr3.at[s], other_z)

    def r4_copy(s):
        return rcopy(s4.at[s], rb.at[zp], sr4.at[s], rr4.at[zp], pair_dev(chunk(s)))

    def compute(s):
        scale = scales[chunk(s)]
        for i in range(nt):
            v = g[s, i].astype(jnp.float32) * scale
            q[pl.ds(i * rows, rows), :] = jnp.clip(v, -QUANT_LIMIT, QUANT_LIMIT).astype(jnp.bfloat16)
        out = jnp.dot(gq[...], q[...], preferred_element_type=jnp.float32)
        part[...] = out.T.reshape(8, 16, wp)
        for i in range(4):
            s1[s, i] = part[2 * i + 1 - c].astype(jnp.bfloat16)

    def finish_r1(s):
        r1_copy(s).wait_recv()
        for zo in range(2):
            a = 2 * zo + 1 - yl
            b = 2 * zo + yl
            s2[s, zo] = (part[2 * a + c] + r1[s, a].astype(jnp.float32)).astype(jnp.bfloat16)
            keep2[zo] = part[2 * b + c] + r1[s, b].astype(jnp.float32)
        r2_copy(s).start()

    def finish_r2(s):
        r2_copy(s).wait_recv()
        s3[s] = (keep2[1 - zq] + r2[s, 1 - zq].astype(jnp.float32)).astype(jnp.bfloat16)
        keep3[s] = keep2[zq] + r2[s, zq].astype(jnp.float32)
        r3_copy(s).start()

    def finish_r3(s):
        r3_copy(s).wait_recv()
        total = keep3[s] + r3[s].astype(jnp.float32)
        s4[s] = total.astype(jnp.bfloat16)
        own_sum[...] = total

    def start_r4(s):
        @pl.when(chunk(s) != zp)
        def _():
            r4_copy(s).start()

    def p2_copy():
        return rcopy(pv, pcore, sp2, rp2, other_core)

    def p3_copy():
        return rcopy(pcore, pylo, sp3, rp3, other_yl)

    def p4_copy():
        return rcopy(pylo, pzz, sp4, rp4, other_z)

    def p5_copy(i):
        return rcopy(pzz, pfar.at[i], sp5.at[i], rp5.at[i], pair_dev((zp + i) % nc))

    def h3_copy(i):
        dst = ch.at[pl.ds(hrow, 8), pl.ds(hcol, LANES)]
        return rcopy(hb, dst, sh3.at[i], rh3.at[i], pair_dev((zp + i) % nc))

    def h3_arrival(i):
        col = pl.multiple_of(((zp + nc - i) % nc) * LANES, LANES)
        dst = ch.at[pl.ds(hrow, 8), pl.ds(col, LANES)]
        return rcopy(hb, dst, sh3.at[i], rh3.at[i], other_core)

    def h4_copy():
        half = ch.at[pl.ds(hrow, 8), :]
        return rcopy(half, half, sh4, rh4, other_core)

    def h4_arrival():
        half = ch.at[pl.ds(pl.multiple_of(8 - hrow, 8), 8), :]
        return rcopy(half, half, sh4, rh4, other_core)

    def side_work(s):
        def p3():
            p2_copy().wait_recv()
            pcore[...] = jnp.maximum(pcore[...], pv[...])
            p3_copy().start()

        def p4():
            p3_copy().wait_recv()
            pylo[...] = jnp.maximum(pylo[...], pcore[...])
            p4_copy().start()

        def far():
            p4_copy().wait_recv()
            pzz[...] = jnp.maximum(pzz[...], pylo[...])
            for i in range(1, nc):
                h3_copy(i).start()
            for i in range(1, nc):
                p5_copy(i).start()

        def h4():
            for i in range(1, nc):
                h3_arrival(i).wait_recv()
            h4_copy().start()

        todo = [(0, p2_copy().start), (1, p3), (2, p4), (tok_step + 1, far), (6, h4)]
        for at, work in todo:
            pl.when(s == min(at, nc - 1))(work)

    def tokens_wait():
        @pl.when(zp < early)
        def _():
            pl.semaphore_wait(tok1, nc - 1 - zp)
            for pp in range(early, nc):
                @pl.when((nc - 1 - pp) % early == zp)
                def _():
                    signal(tok2, pair_dev(pp))

        @pl.when(zp >= early)
        def _():
            pl.semaphore_wait(tok2, 1)

    def step(s, carry):
        @pl.when(s + 3 < nc)
        def _():
            stage_own(s + 3)

        @pl.when(s >= 1)
        def _():
            finish_r1(s - 1)

        @pl.when(s + 2 < nc)
        def _():
            stage_partner(s + 2)
            stage_far_own(s + 2)

        @pl.when(s + 1 < nc)
        def _():
            stage_far_other(s + 1)

        @pl.when(s >= 2)
        def _():
            finish_r3(s - 2)

        @pl.when(s == tok_step)
        def _():
            tokens_wait()
            for i in range(max(tok_step - 2, 0)):
                start_r4(i)

        @pl.when(jnp.logical_and(s >= tok_step, s >= 2))
        def _():
            start_r4(s - 2)

        stage_finish(s)
        compute(s)
        r1_copy(s).start()

        @pl.when(s >= 1)
        def _():
            finish_r2(s - 1)

        side_work(s)
        return carry

    lax.fori_loop(0, nc, step, 0)
    last = nc - 1
    finish_r1(last)
    if nc > 1:
        finish_r3(last - 1)
        start_r4(last - 1)
    h4_arrival().wait_recv()
    hist_out[...] = ch[...]
    finish_r2(last)
    top = pzz[...]
    for i in range(1, nc):
        p5_copy(i).wait_recv()
        top = jnp.maximum(top, pfar[i])
    for k in range(nc):
        peak_out[:, k * LANES : (k + 1) * LANES] = top[k : k + 1, :]
    for k in range(wp // LANES):
        n = min(width - k * LANES, LANES)
        gpeak_out[:, k * LANES : k * LANES + n] = top[8 + k : 9 + k, :n]
    finish_r3(last)

    total = own_sum[...]
    for i in range(1, nc):
        frm = (zp + i) % nc
        rcopy(rb.at[frm], rb.at[frm], sr4.at[0], rr4.at[frm], other_core).wait_recv()
        total = total + rb[frm].astype(jnp.float32)
    sum_out[...] = total[:, :width]

    def drain_gather(s):
        y_copy(s).wait_send()
        for d in range(2):
            xo_copy(s, d).wait_send()
            xp_copy(s, d).wait_send()
        far_own(s, 0).wait_send()
        cond(kind_a(s), lambda: far_other(s, 0).wait_send())
        cond(kind_c(s), lambda: y2_copy(s).wait_send())

    def drain(s, carry):
        drain_gather(s)
        r1_copy(s).wait_send()
        r2_copy(s).wait_send()
        r3_copy(s).wait_send()

        @pl.when(chunk(s) != zp)
        def _():
            r4_copy(s).wait_send()

        return carry

    drain_gather(nc)
    lax.fori_loop(0, nc, drain, 0)
    h4_copy().wait_send()
    p2_copy().wait_send()
    p3_copy().wait_send()
    p4_copy().wait_send()
    for i in range(1, nc):
        h3_copy(i).wait_send()
        p5_copy(i).wait_send()


def fused(acts, grads, ahist, ghist, owner, nz, nx):
    rows, model = acts.shape
    width, tokens = grads.shape
    nc, nt = nz // 2, 2 * nx
    wp = -(-width // LANES) * LANES
    f32, bf16 = jnp.float32, jnp.bfloat16
    dma = pltpu.SemaphoreType.DMA
    vm = pltpu.VMEM
    scratch = [
        vm((nc, nt, rows, LANES), bf16),
        vm((rows, model), bf16),
        vm((width, tokens), bf16),
        vm((wp, tokens), bf16),
        vm((tokens, LANES), bf16),
        vm((1, 16, model), f32),
        vm((16, width), f32),
        vm((1, model), jnp.int32),
        vm((wp, LANES), f32),
        vm((wp, LANES), f32),
        vm((nc, 1, LANES), f32),
        vm((16, model), f32),
        vm((nt, 24, LANES), f32),
        vm((8, LANES), f32),
        vm((16, model), f32),
        vm((16, LANES), f32),
        vm((16, LANES), f32),
        vm((16, LANES), f32),
        vm((16, LANES), f32),
        vm((nc, 16, LANES), f32),
        vm((8, 16, wp), f32),
        vm((nc, 4, 16, wp), bf16),
        vm((nc, 4, 16, wp), bf16),
        vm((nc, 2, 16, wp), bf16),
        vm((nc, 2, 16, wp), bf16),
        vm((2, 16, wp), f32),
        vm((nc, 16, wp), bf16),
        vm((nc, 16, wp), bf16),
        vm((nc, 16, wp), f32),
        vm((nc, 16, wp), bf16),
        vm((nc, 16, wp), bf16),
        vm((16, wp), f32),
        dma((nc,)), dma((5,)),
        dma((nc + 1,)), dma((nc + 1,)),
        dma((nc + 1, 2)), dma((nc + 1, 2)), dma((nc + 1, 2)), dma((nc + 1, 2)),
        dma((nc + 1, 2)), dma((nc + 1, 2)), dma((nc + 1,)), dma((nc + 1,)),
        dma((nc,)), dma((nc,)), dma, dma,
        dma, dma, dma, dma, dma, dma, dma((nc,)), dma((nc,)),
        dma((nc,)), dma((nc,)), dma((nc,)), dma((nc,)),
        dma((nc,)), dma((nc,)), dma((nc,)), dma((nc,)),
        pltpu.SemaphoreType.REGULAR, pltpu.SemaphoreType.REGULAR,
    ]
    vspec = pl.BlockSpec(memory_space=pltpu.VMEM)
    anyspec = pl.BlockSpec(memory_space=pl.ANY)
    return pl.pallas_call(
        functools.partial(kernel, nz, nx),
        out_shape=[
            jax.ShapeDtypeStruct((16, width), f32),
            jax.ShapeDtypeStruct((16, model), f32),
            jax.ShapeDtypeStruct((1, model), f32),
            jax.ShapeDtypeStruct((1, width), f32),
            jax.ShapeDtypeStruct((1, model), f32),
            jax.ShapeDtypeStruct((1, width), f32),
        ],
        in_specs=[anyspec] * 5,
        out_specs=[vspec] * 6,
        scratch_shapes=scratch,
        compiler_params=pltpu.CompilerParams(
            collective_id=0, has_side_effects=True, vmem_limit_bytes=60 * 1024 * 1024
        ),
    )(acts, grads, ahist, ghist, owner)


def body(nz, nx, activations, gradients, act_history, grad_history, owner_rank, history_slot):
    model = act_history.shape[2]
    width = gradients.shape[1]
    my_rank = lax.axis_index("tensor")
    summed, current, act_peak, grad_peak, act_scale, grad_scale = fused(
        activations, gradients.T, act_history, grad_history, owner_rank.reshape(1, model), nz, nx
    )
    grad_factor = 1.0 / math.sqrt(gradients.shape[0] * lax.axis_size("dp"))
    row_base = lax.axis_index("dp") * 16
    row_scale = lax.dynamic_slice(act_scale, (0, row_base), (1, 16)).reshape(16, 1)
    weight_grad = summed / (row_scale * grad_scale) * grad_factor
    act_slots = history_slot[:model]
    grad_slots = lax.dynamic_slice_in_dim(history_slot, model + my_rank * width, width, 0)

    def place(history, peaks, slots):
        at = lax.broadcasted_iota(jnp.int32, history.shape, 0)
        return jnp.where(at == slots[None, :], peaks, history)

    act_history_out = place(current, act_peak, act_slots)[None]
    grad_history_out = place(grad_history, grad_peak, grad_slots)
    return (weight_grad, act_history_out, grad_history_out)


def solution(mesh):
    nz = mesh.shape["dp"] // 4
    nx = mesh.shape["tensor"] // 2
    placed = (
        P(("dp", "tensor"), None),
        P("dp", "tensor"),
        P("tensor", None, None),
        P(None, "tensor"),
        P(),
        P(),
    )
    return jax.shard_map(
        functools.partial(body, nz, nx),
        mesh=mesh,
        in_specs=placed,
        out_specs=(P("dp", "tensor"), P("tensor", None, None), P(None, "tensor")),
        check_vma=False,
    )
```

```python
import functools
import math

import jax
import jax.numpy as jnp
from jax import lax
from jax.experimental import pallas as pl
from jax.experimental.pallas import tpu as pltpu
from jax.sharding import PartitionSpec as P

QUANT_LIMIT = 448.0
SCALE_FLOOR = 0.25
LANES = 128
BLOCK = 64
AHEAD = 4
DIRECT = 1
MESH = pl.DeviceIdType.MESH


def kernel(
    nz, nx, factor, acts, grads, ahist, ghist, owner, slots,
    wgrad_out, hist_out, ghist_out,
    g, acol, graw, gq, q, ah, gh, ow, sl, gsl, peak_row, gpeak_row, gcol, gpk, scales, mh, small, hb, ch,
    pv, pcore, pylo, pzz, pfar,
    part, s1, r1, s2, r2, keep2, s4, rb, own_sum, sd, rd, keepd,
    ld_g, ld_x,
    sy, ry, sxo, rxo, sxp, rxp, sf, rf, sy2, ry2,
    sh3, rh3, sh4, rh4, sp2, rp2, sp3, rp3, sp4, rp4, sp5, rp5,
    sr1, rr1, sr2, rr2, sr4, rr4, srd, rrd, tok1, tok2,
):
    nc = nz // 2
    nt = 2 * nx
    early = max(3 * nc // 8, 1)
    tok_step = min(1, nc - 1)
    chain = nc - min(DIRECT, nc)
    rows = acts.shape[0]
    width, tokens = grads.shape
    wp = gq.shape[0]
    t = lax.axis_index("tensor")
    dpi = lax.axis_index("dp")
    x, yh = t // 2, t % 2
    z, yl, c = dpi // 4, (dpi // 2) % 2, dpi % 2
    zp, zq = z // 2, z % 2
    xr, xl, xf = (x + 1) % nx, (x + nx - 1) % nx, (x + 2) % nx
    yo = 1 - yh

    def tensor_dev(tt):
        return {"dp": dpi, "tensor": tt}

    def dp_dev(zz, yy, cc):
        return {"dp": zz * 4 + yy * 2 + cc, "tensor": t}

    def pair_dev(pp):
        return dp_dev(2 * pp + zq, yl, c)

    def rcopy(src, dst, ss, rs, device):
        return pltpu.make_async_remote_copy(
            src_ref=src, dst_ref=dst, send_sem=ss, recv_sem=rs,
            device_id=device, device_id_type=MESH,
        )

    def signal(sem, device):
        pl.semaphore_signal(sem, inc=1, device_id=device, device_id_type=MESH)

    def chunk(s):
        hf = nc // 2
        late = s // hf
        j = 2 * hf - 1 - s
        high = zp // hf
        u = high * (zp - hf) + (1 - high) * (hf - 1 - zp)
        flip = (u + j) % 2 + 2 * ((u // 2 + j // 2) % 2)
        return (1 - late) * s + late * (hf + flip % hf)

    partner_y = tensor_dev(2 * x + yo)
    right = tensor_dev(2 * xr + yh)
    left = tensor_dev(2 * xl + yh)
    other_core = dp_dev(z, yl, 1 - c)
    other_yl = dp_dev(z, 1 - yl, c)
    other_z = dp_dev(2 * zp + 1 - zq, yl, c)

    def cube_index(i):
        return (zq + i // 4) % 2, (yl + i // 2 % 2) % 2, (c + i % 2) % 2

    def cube_dev(i):
        zz, yy, cc = cube_index(i)
        return dp_dev(2 * zp + zz, yy, cc)

    def load_g(s):
        col = pl.multiple_of(chunk(s) * LANES, LANES)
        return pltpu.make_async_copy(acts.at[:, pl.ds(col, LANES)], g.at[s, t], ld_g.at[s])

    loads = [
        pltpu.make_async_copy(src, dst, ld_x.at[i])
        for i, (src, dst) in enumerate(
            [(ahist, ah), (owner, ow), (ghist, gh), (acts, acol), (grads, graw), (slots, sl)]
        )
    ]
    loads[0].start()
    loads[1].start()
    for s in range(nc):
        load_g(s).start()
    for i in (3, 2, 4, 5):
        loads[i].start()

    bar = pltpu.get_barrier_semaphore()
    for device in (partner_y, right, left):
        signal(bar, device)
    for i in range(1, 8):
        signal(bar, cube_dev(i))
    for i in range(1, nc):
        @pl.when(jnp.logical_and(zp < early, zp + i < nc))
        def _():
            signal(bar, pair_dev(zp + i))

    def to_rows(vec, at, count):
        for k in range(count):
            small[t, at + k : at + k + 1, :] = vec[:, k * LANES : (k + 1) * LANES]

    loads[0].wait()
    loads[1].wait()
    held = jnp.where(ow[...] == t, ah[0], jnp.float32(0.0))
    mh[...] = held
    to_rows(jnp.max(held, axis=0, keepdims=True), 0, nc)
    hcol = pl.multiple_of(zp * LANES, LANES)
    hrow = pl.multiple_of(c * 8, 8)
    small[t, 8:16, :] = mh[pl.ds(hrow, 8), pl.ds(hcol, LANES)]
    loads[3].wait()
    to_rows(jnp.max(jnp.abs(acol[...].astype(jnp.float32)), axis=0, keepdims=True), 16, nc)

    pl.semaphore_wait(bar, 10 + jnp.minimum(zp, early))
    for i in range(early):
        @pl.when(i < zp)
        def _():
            signal(tok1, pair_dev(i))

    def at_slot(s, xx, yy):
        if isinstance(s, int) and s == nc:
            return small.at[2 * xx + yy]
        return g.at[s, 2 * xx + yy]

    def y_copy(s):
        return rcopy(at_slot(s, x, yh), at_slot(s, x, yh), sy.at[s], ry.at[s], partner_y)

    def y_arrival(s):
        return rcopy(at_slot(s, x, yo), at_slot(s, x, yo), sy.at[s], ry.at[s], partner_y)

    def xo_copy(s, d):
        a = at_slot(s, x, yh)
        return rcopy(a, a, sxo.at[s, d], rxo.at[s, d], right if d == 0 else left)

    def xo_arrival(s, d):
        a = at_slot(s, xl if d == 0 else xr, yh)
        return rcopy(a, a, sxo.at[s, d], rxo.at[s, d], right)

    def xp_copy(s, d):
        a = at_slot(s, x, yo)
        return rcopy(a, a, sxp.at[s, d], rxp.at[s, d], right if d == 0 else left)

    def xp_arrival(s, d):
        a = at_slot(s, xl if d == 0 else xr, yo)
        return rcopy(a, a, sxp.at[s, d], rxp.at[s, d], right)

    def far_own(s, d):
        a = at_slot(s, xl if d == 0 else xr, yh)
        return rcopy(a, a, sf.at[s, 0], rf.at[s, 0], right if d == 0 else left)

    def far_own_arrival(s):
        a = at_slot(s, xf, yh)
        return rcopy(a, a, sf.at[s, 0], rf.at[s, 0], right)

    def far_other(s, d):
        a = at_slot(s, xl if d == 0 else xr, yo)
        return rcopy(a, a, sf.at[s, 1], rf.at[s, 1], right if d == 0 else left)

    def far_other_arrival(s):
        a = at_slot(s, xf, yo)
        return rcopy(a, a, sf.at[s, 1], rf.at[s, 1], right)

    def y2_copy(s):
        a = at_slot(s, xf, yh)
        return rcopy(a, a, sy2.at[s], ry2.at[s], partner_y)

    def y2_arrival(s):
        a = at_slot(s, xf, yo)
        return rcopy(a, a, sy2.at[s], ry2.at[s], partner_y)

    def cond(pred, work):
        if isinstance(pred, bool):
            if pred:
                work()
        else:
            pl.when(pred)(work)

    def kind_a(s):
        if isinstance(s, int) and s == nc:
            return True
        return s % 1 == 0

    def kind_c(s):
        if isinstance(s, int) and s == nc:
            return False
        return s % 1 != 0

    def stage_own(s):
        xo_copy(s, 0).start()
        xo_copy(s, 1).start()

    def stage_partner(s):
        y_arrival(s).wait_recv()
        xp_copy(s, 0).start()
        xp_copy(s, 1).start()

    def stage_far_own(s):
        def go(d):
            xo_arrival(s, d).wait_recv()
            far_own(s, d).start()

        cond(s % 2 == 0, lambda: go(0))
        cond(s % 2 == 1, lambda: go(1))

    def stage_far_other(s):
        def kind_a_work():
            def go(d):
                xp_arrival(s, d).wait_recv()
                far_other(s, d).start()

            cond(s % 2 == 0, lambda: go(1))
            cond(s % 2 == 1, lambda: go(0))

        def kind_c_work():
            far_own_arrival(s).wait_recv()
            y2_copy(s).start()

        cond(kind_a(s), kind_a_work)
        cond(kind_c(s), kind_c_work)

    def stage_finish(s):
        def even():
            xo_arrival(s, 1).wait_recv()

        def odd():
            xo_arrival(s, 0).wait_recv()

        cond(s % 2 == 0, even)
        cond(s % 2 == 1, odd)

        def kind_a_work():
            cond(s % 2 == 0, lambda: xp_arrival(s, 0).wait_recv())
            cond(s % 2 == 1, lambda: xp_arrival(s, 1).wait_recv())
            far_own_arrival(s).wait_recv()
            far_other_arrival(s).wait_recv()

        def kind_c_work():
            xp_arrival(s, 0).wait_recv()
            xp_arrival(s, 1).wait_recv()
            y2_arrival(s).wait_recv()

        cond(kind_a(s), kind_a_work)
        cond(kind_c(s), kind_c_work)

    y_copy(nc).start()
    stage_own(nc)
    for s in range(nc):
        load_g(s).wait()
        if s < min(4, AHEAD + 1):
            y_copy(s).start()
        if s < min(3, AHEAD):
            stage_own(s)

    def p2_copy():
        return rcopy(pv, pcore, sp2, rp2, other_core)

    loads[2].wait()
    gscale = QUANT_LIMIT / jnp.maximum(jnp.max(gh[...], axis=0, keepdims=True), SCALE_FLOOR)
    pad = jnp.zeros((1, wp - width), jnp.float32)
    gcol[...] = jnp.broadcast_to(jnp.concatenate([gscale, pad], axis=1), (LANES, wp)).T
    loads[4].wait()
    loads[5].wait()
    for i in range(nt):
        at = nc * LANES + i * width

        @pl.when(t == i)
        def _():
            gsl[...] = sl[:, at : at + width]


    def quant_rows(at, count):
        scale = gcol[at, :]
        top = jnp.zeros((count, LANES), jnp.float32)
        for j in range(tokens // LANES):
            v = graw[at, j * LANES : (j + 1) * LANES].astype(jnp.float32)
            gq[at, j * LANES : (j + 1) * LANES] = jnp.clip(
                v * scale, -QUANT_LIMIT, QUANT_LIMIT
            ).astype(jnp.bfloat16)
            top = jnp.maximum(top, jnp.abs(v))
        gpk[at, :] = top

    def quant_block(i, carry):
        quant_rows(pl.ds(pl.multiple_of(i * BLOCK, BLOCK), BLOCK), BLOCK)
        return carry

    full = width // BLOCK
    for j in range(1, AHEAD):
        if j <= 3:
            lax.fori_loop((j - 1) * full // 3, j * full // 3, quant_block, 0)
        if j == 1:
            stage_partner(nc)
            stage_far_own(nc)
        if j == 2:
            stage_far_other(nc)
        if j - 1 < nc:
            stage_partner(j - 1)
            stage_far_own(j - 1)
        if 0 <= j - 2 < min(AHEAD - 3, nc):
            stage_far_other(j - 2)
        if j + 3 < min(AHEAD + 1, nc):
            y_copy(j + 3).start()
        if j + 2 < min(AHEAD, nc):
            stage_own(j + 2)
    if width > full * BLOCK:
        quant_rows(slice(full * BLOCK, width), width - full * BLOCK)
    gq[width:, :] = jnp.zeros((wp - width, tokens), jnp.bfloat16)
    gpk[width:, :] = jnp.zeros((wp - width, LANES), jnp.float32)
    gpeak = jnp.max(gpk[...].T, axis=0, keepdims=True)

    stage_finish(nc)
    total_small = small[0]
    apeak = small[0, 16:24, :]
    for i in range(1, nt):
        total_small = total_small + small[i]
        apeak = jnp.maximum(apeak, small[i, 16:24, :])
    ascale = QUANT_LIMIT / jnp.maximum(total_small[0:8, :], SCALE_FLOOR)
    for k in range(nc):
        scales[k] = ascale[k : k + 1, :]
    hb[...] = total_small[8:16, :]
    ch[pl.ds(hrow, 8), pl.ds(hcol, LANES)] = total_small[8:16, :]
    pv[0:8, :] = apeak
    for k in range(wp // LANES):
        pv[8 + k : 9 + k, :] = gpeak[:, k * LANES : (k + 1) * LANES]
    pv[8 + wp // LANES :, :] = jnp.zeros((8 - wp // LANES, LANES), jnp.float32)
    p2_copy().start()

    def r1_copy(s):
        return rcopy(s1.at[s], r1.at[s], sr1.at[s], rr1.at[s], other_core)

    def r4_copy(s):
        return rcopy(s4.at[s], rb.at[zp], sr4.at[s], rr4.at[zp], pair_dev(chunk(s)))

    def compute(s):
        scale = scales[chunk(s)]
        for i in range(nt):
            v = g[s, i].astype(jnp.float32) * scale
            q[pl.ds(i * rows, rows), :] = jnp.clip(v, -QUANT_LIMIT, QUANT_LIMIT).astype(jnp.bfloat16)
        out = jnp.dot(gq[...], q[...], preferred_element_type=jnp.float32)
        part[...] = out.T.reshape(8, 16, wp)

    def start_r1(s):
        for i in range(4):
            s1[s, i] = part[2 * i + 1 - c].astype(jnp.bfloat16)
        r1_copy(s).start()

    def direct_copy(s, i):
        zz, yy, cc = cube_index(i)
        k = s - chain
        return rcopy(
            sd.at[k, zz * 4 + yy * 2 + cc], rd.at[k, i], srd.at[k, i], rrd.at[k, i], cube_dev(i)
        )

    def start_direct(s):
        sd[s - chain] = part[...].astype(jnp.bfloat16)
        keepd[s - chain] = part[zq * 4 + yl * 2 + c]
        for i in range(1, 8):
            direct_copy(s, i).start()

    def finish_direct(s):
        total = keepd[s - chain]
        for i in range(1, 8):
            direct_copy(s, i).wait_recv()
            total = total + rd[s - chain, i].astype(jnp.float32)
        emit(s, total)

    def quad_copy(s, i):
        zz, yy, _ = cube_index(2 * i)
        return rcopy(
            s2.at[s, i], r2.at[s, i], sr2.at[s, i], rr2.at[s, i], dp_dev(2 * zp + zz, yy, c)
        )

    def finish_r1(s):
        r1_copy(s).wait_recv()
        for i in range(4):
            zz, yy, _ = cube_index(2 * i)
            k = 2 * zz + yy
            total = part[2 * k + c] + r1[s, k].astype(jnp.float32)
            if i == 0:
                keep2[s % 2] = total
            else:
                s2[s, i] = total.astype(jnp.bfloat16)
        for i in range(1, 4):
            quad_copy(s, i).start()

    def finish_quad(s):
        total = keep2[s % 2]
        for i in range(1, 4):
            quad_copy(s, i).wait_recv()
            total = total + r2[s, i].astype(jnp.float32)
        emit(s, total)

    def emit(s, total):
        s4[s] = total.astype(jnp.bfloat16)

        @pl.when(chunk(s) == zp)
        def _():
            own_sum[...] = total

        @pl.when(chunk(s) != zp)
        def _():
            r4_copy(s).start()

    def p3_copy():
        return rcopy(pcore, pylo, sp3, rp3, other_yl)

    def p4_copy():
        return rcopy(pylo, pzz, sp4, rp4, other_z)

    def p5_copy(i):
        return rcopy(pzz, pfar.at[i], sp5.at[i], rp5.at[i], pair_dev((zp + i) % nc))

    def h3_copy(i):
        dst = ch.at[pl.ds(hrow, 8), pl.ds(hcol, LANES)]
        return rcopy(hb, dst, sh3.at[i], rh3.at[i], pair_dev((zp + i) % nc))

    def h3_arrival(i):
        col = pl.multiple_of(((zp + nc - i) % nc) * LANES, LANES)
        dst = ch.at[pl.ds(hrow, 8), pl.ds(col, LANES)]
        return rcopy(hb, dst, sh3.at[i], rh3.at[i], other_core)

    def h4_copy():
        half = ch.at[pl.ds(hrow, 8), :]
        return rcopy(half, half, sh4, rh4, other_core)

    def h4_arrival():
        half = ch.at[pl.ds(pl.multiple_of(8 - hrow, 8), 8), :]
        return rcopy(half, half, sh4, rh4, other_core)

    def side_work(s):
        def p3():
            p2_copy().wait_recv()
            pcore[...] = jnp.maximum(pcore[...], pv[...])
            p3_copy().start()

        def p4():
            p3_copy().wait_recv()
            pylo[...] = jnp.maximum(pylo[...], pcore[...])
            p4_copy().start()

        def far():
            p4_copy().wait_recv()
            pzz[...] = jnp.maximum(pzz[...], pylo[...])
            for i in range(1, nc):
                h3_copy(i).start()
            for i in range(1, nc):
                p5_copy(i).start()

        todo = [(0, p3), (1, p4), (2, far)]
        for at, work in todo:
            pl.when(s == min(at, nc - 1))(work)

    def tokens_wait():
        @pl.when(zp < early)
        def _():
            pl.semaphore_wait(tok1, nc - 1 - zp)
            for pp in range(early, nc):
                @pl.when((nc - 1 - pp) % early == zp)
                def _():
                    signal(tok2, pair_dev(pp))

        @pl.when(zp >= early)
        def _():
            pl.semaphore_wait(tok2, 1)

    def step(s, carry):
        @pl.when(s + AHEAD + 1 < nc)
        def _():
            y_copy(s + AHEAD + 1).start()

        @pl.when(s + AHEAD < nc)
        def _():
            stage_own(s + AHEAD)

        @pl.when(jnp.logical_and(s >= 1, s - 1 < chain))
        def _():
            finish_r1(s - 1)

        stage_finish(s)
        compute(s)

        @pl.when(s < chain)
        def _():
            start_r1(s)

        @pl.when(s >= chain)
        def _():
            start_direct(s)

        @pl.when(jnp.logical_and(s == 0, AHEAD - 3 < nc))
        def _():
            stage_far_other(s + AHEAD - 3)

        @pl.when(s + AHEAD - 1 < nc)
        def _():
            stage_partner(s + AHEAD - 1)
            stage_far_own(s + AHEAD - 1)

        @pl.when(s == tok_step)
        def _():
            tokens_wait()

        @pl.when(jnp.logical_and(s >= 2, s - 2 < chain))
        def _():
            finish_quad(s - 2)

        @pl.when(s + AHEAD - 2 < nc)
        def _():
            stage_far_other(s + AHEAD - 2)

        @pl.when(s >= chain + 1)
        def _():
            finish_direct(s - 1)

        side_work(s)
        return carry

    lax.fori_loop(0, nc, step, 0)
    last = nc - 1
    for i in range(1, nc):
        h3_arrival(i).wait_recv()
    h4_copy().start()
    if 0 <= last - 1 < chain:
        finish_quad(last - 1)
    top = pzz[...]
    for i in range(1, nc):
        p5_copy(i).wait_recv()
        top = jnp.maximum(top, pfar[i])
    for k in range(nc):
        peak_row[:, k * LANES : (k + 1) * LANES] = top[k : k + 1, :]
    for k in range(wp // LANES):
        n = min(width - k * LANES, LANES)
        gpeak_row[:, k * LANES : k * LANES + n] = top[8 + k : 9 + k, :n]
    hist_row = lax.broadcasted_iota(jnp.int32, ghist_out.shape, 0)
    ghist_out[...] = jnp.where(hist_row == gsl[...], gpeak_row[...], gh[...])
    h4_arrival().wait_recv()
    hist_row = lax.broadcasted_iota(jnp.int32, hist_out.shape, 0)
    hist_out[...] = jnp.where(hist_row == sl[:, : nc * LANES], peak_row[...], ch[...])
    lane = lax.broadcasted_iota(jnp.int32, (16, LANES), 1)
    row = lax.broadcasted_iota(jnp.int32, (16, LANES), 0)
    mine = lane == row + (zq * 4 + yl * 2 + c) * 16
    row_scale = jnp.sum(jnp.where(mine, scales[zp], jnp.float32(0.0)), axis=1, keepdims=True)
    gscale = QUANT_LIMIT / jnp.maximum(jnp.max(gh[...], axis=0, keepdims=True), SCALE_FLOOR)
    finish_direct(last)

    total = own_sum[...]
    for i in range(1, nc):
        frm = (zp + i) % nc
        rcopy(rb.at[frm], rb.at[frm], sr4.at[0], rr4.at[frm], other_core).wait_recv()
        total = total + rb[frm].astype(jnp.float32)
    wgrad_out[...] = total[:, :width] / (row_scale * gscale) * factor

    def drain_gather(s):
        y_copy(s).wait_send()
        for d in range(2):
            xo_copy(s, d).wait_send()
            xp_copy(s, d).wait_send()
        far_own(s, 0).wait_send()
        cond(kind_a(s), lambda: far_other(s, 0).wait_send())
        cond(kind_c(s), lambda: y2_copy(s).wait_send())

    def drain(s, carry):
        drain_gather(s)

        @pl.when(s < chain)
        def _():
            r1_copy(s).wait_send()
            for i in range(1, 4):
                quad_copy(s, i).wait_send()

        @pl.when(chunk(s) != zp)
        def _():
            r4_copy(s).wait_send()

        return carry

    drain_gather(nc)
    lax.fori_loop(0, nc, drain, 0)
    for s in range(chain, nc):
        for i in range(1, 8):
            direct_copy(s, i).wait_send()
    h4_copy().wait_send()
    p2_copy().wait_send()
    p3_copy().wait_send()
    p4_copy().wait_send()
    for i in range(1, nc):
        h3_copy(i).wait_send()
        p5_copy(i).wait_send()


def fused(acts, grads, ahist, ghist, owner, slots, nz, nx, factor):
    rows, model = acts.shape
    width, tokens = grads.shape
    nc, nt = nz // 2, 2 * nx
    wp = -(-width // LANES) * LANES
    f32, bf16 = jnp.float32, jnp.bfloat16
    dma = pltpu.SemaphoreType.DMA
    vm = pltpu.VMEM
    scratch = [
        vm((nc, nt, rows, LANES), bf16),
        vm((rows, model), bf16),
        vm((width, tokens), bf16),
        vm((wp, tokens), bf16),
        vm((tokens, LANES), bf16),
        vm((1, 16, model), f32),
        vm((16, width), f32),
        vm((1, model), jnp.int32),
        vm(slots.shape, jnp.int32),
        vm((1, width), jnp.int32),
        vm((1, model), f32),
        vm((1, width), f32),
        vm((wp, LANES), f32),
        vm((wp, LANES), f32),
        vm((nc, 1, LANES), f32),
        vm((16, model), f32),
        vm((nt, 24, LANES), f32),
        vm((8, LANES), f32),
        vm((16, model), f32),
        vm((16, LANES), f32),
        vm((16, LANES), f32),
        vm((16, LANES), f32),
        vm((16, LANES), f32),
        vm((nc, 16, LANES), f32),
        vm((8, 16, wp), f32),
        vm((nc, 4, 16, wp), bf16),
        vm((nc, 4, 16, wp), bf16),
        vm((nc, 4, 16, wp), bf16),
        vm((nc, 4, 16, wp), bf16),
        vm((2, 16, wp), f32),
        vm((nc, 16, wp), bf16),
        vm((nc, 16, wp), bf16),
        vm((16, wp), f32),
        vm((DIRECT, 8, 16, wp), bf16),
        vm((DIRECT, 8, 16, wp), bf16),
        vm((DIRECT, 16, wp), f32),
        dma((nc,)), dma((6,)),
        dma((nc + 1,)), dma((nc + 1,)),
        dma((nc + 1, 2)), dma((nc + 1, 2)), dma((nc + 1, 2)), dma((nc + 1, 2)),
        dma((nc + 1, 2)), dma((nc + 1, 2)), dma((nc + 1,)), dma((nc + 1,)),
        dma((nc,)), dma((nc,)), dma, dma,
        dma, dma, dma, dma, dma, dma, dma((nc,)), dma((nc,)),
        dma((nc,)), dma((nc,)), dma((nc, 4)), dma((nc, 4)), dma((nc,)), dma((nc,)),
        dma((DIRECT, 8)), dma((DIRECT, 8)),
        pltpu.SemaphoreType.REGULAR, pltpu.SemaphoreType.REGULAR,
    ]
    vspec = pl.BlockSpec(memory_space=pltpu.VMEM)
    anyspec = pl.BlockSpec(memory_space=pl.ANY)
    return pl.pallas_call(
        functools.partial(kernel, nz, nx, factor),
        out_shape=[
            jax.ShapeDtypeStruct((16, width), f32),
            jax.ShapeDtypeStruct((16, model), f32),
            jax.ShapeDtypeStruct((16, width), f32),
        ],
        in_specs=[anyspec] * 6,
        out_specs=[vspec] * 3,
        scratch_shapes=scratch,
        compiler_params=pltpu.CompilerParams(
            collective_id=0, has_side_effects=True, vmem_limit_bytes=54600 * 1024
        ),
    )(acts, grads, ahist, ghist, owner, slots)


def body(nz, nx, activations, gradients, act_history, grad_history, owner_rank, history_slot):
    factor = 1.0 / math.sqrt(gradients.shape[0] * lax.axis_size("dp"))
    weight_grad, act_history_out, grad_history_out = fused(
        activations, gradients.T, act_history, grad_history,
        owner_rank.reshape(1, -1), history_slot.reshape(1, -1), nz, nx, factor,
    )
    return (weight_grad, act_history_out[None], grad_history_out)


def solution(mesh):
    nz = mesh.shape["dp"] // 4
    nx = mesh.shape["tensor"] // 2
    placed = (
        P(("dp", "tensor"), None),
        P("dp", "tensor"),
        P("tensor", None, None),
        P(None, "tensor"),
        P(),
        P(),
    )
    return jax.shard_map(
        functools.partial(body, nz, nx),
        mesh=mesh,
        in_specs=placed,
        out_specs=(P("dp", "tensor"), P("tensor", None, None), P(None, "tensor")),
        check_vma=False,
    )
```

```python
import functools
import math

import jax
import jax.numpy as jnp
from jax import lax
from jax.experimental import pallas as pl
from jax.experimental.pallas import tpu as pltpu
from jax.sharding import PartitionSpec as P

QUANT_LIMIT = 448.0
SCALE_FLOOR = 0.25
LANES = 128
BLOCK = 64
AHEAD = 4
MESH = pl.DeviceIdType.MESH


def kernel(
    nz, nx, factor, acts, grads, ahist, ghist, owner, slots,
    wgrad_out, hist_out, ghist_out,
    g, acol, graw, gq, q, ah, gh, ow, sl, gsl, peak_row, gpeak_row, gcol, gpk, scales, mh, small, hb, ch,
    pv, pcore, pylo, pzz, pfar,
    part, s1, r1, s2, r2, keep2, s4, rb, own_sum,
    ld_g, ld_x,
    sg, rg,
    sh3, rh3, sh4, rh4, sp2, rp2, sp3, rp3, sp4, rp4, sp5, rp5,
    sr1, rr1, sr2, rr2, sr4, rr4, tok1, tok2,
):
    nc = nz // 2
    nt = 2 * nx
    early = max(3 * nc // 8, 1)
    tok_step = min(1, nc - 1)
    rows = acts.shape[0]
    width, tokens = grads.shape
    wp = gq.shape[0]
    t = lax.axis_index("tensor")
    dpi = lax.axis_index("dp")
    x, yh = t // 2, t % 2
    z, yl, c = dpi // 4, (dpi // 2) % 2, dpi % 2
    zp, zq = z // 2, z % 2
    xr, xl, xf = (x + 1) % nx, (x + nx - 1) % nx, (x + 2) % nx
    yo = 1 - yh

    def tensor_dev(tt):
        return {"dp": dpi, "tensor": tt}

    def dp_dev(zz, yy, cc):
        return {"dp": zz * 4 + yy * 2 + cc, "tensor": t}

    def pair_dev(pp):
        return dp_dev(2 * pp + zq, yl, c)

    def rcopy(src, dst, ss, rs, device):
        return pltpu.make_async_remote_copy(
            src_ref=src, dst_ref=dst, send_sem=ss, recv_sem=rs,
            device_id=device, device_id_type=MESH,
        )

    def signal(sem, device):
        pl.semaphore_signal(sem, inc=1, device_id=device, device_id_type=MESH)

    def chunk(s):
        hf = nc // 2
        late = s // hf
        j = 2 * hf - 1 - s
        high = zp // hf
        u = high * (zp - hf) + (1 - high) * (hf - 1 - zp)
        flip = (u + j) % 2 + 2 * ((u // 2 + j // 2) % 2)
        return (1 - late) * s + late * (hf + flip % hf)

    partner_y = tensor_dev(2 * x + yo)
    right = tensor_dev(2 * xr + yh)
    left = tensor_dev(2 * xl + yh)
    other_core = dp_dev(z, yl, 1 - c)
    other_yl = dp_dev(z, 1 - yl, c)
    other_z = dp_dev(2 * zp + 1 - zq, yl, c)

    def cube_index(i):
        return (zq + i // 4) % 2, (yl + i // 2 % 2) % 2, (c + i % 2) % 2

    def cube_dev(i):
        zz, yy, cc = cube_index(i)
        return dp_dev(2 * zp + zz, yy, cc)

    def load_g(s):
        col = pl.multiple_of(chunk(s) * LANES, LANES)
        return pltpu.make_async_copy(
            acts.at[:, pl.ds(col, LANES)], g.at[s * nt + t], ld_g.at[min(s, 1)]
        )

    loads = [
        pltpu.make_async_copy(src, dst, ld_x.at[i])
        for i, (src, dst) in enumerate(
            [(ahist, ah), (owner, ow), (ghist, gh), (acts, acol), (grads, graw), (slots, sl.at[0])]
        )
    ]
    bar = pltpu.get_barrier_semaphore()
    for device in (partner_y, right, left):
        signal(bar, device)
    for i in range(1, 8):
        signal(bar, cube_dev(i))
    for i in range(1, nc):
        @pl.when(jnp.logical_and(zp < early, zp + i < nc))
        def _():
            signal(bar, pair_dev(zp + i))

    load_g(0).start()
    for i in (0, 1, 3):
        loads[i].start()
    for s in range(1, nc):
        load_g(s).start()
    for i in (2, 4, 5):
        loads[i].start()

    def to_rows(vec, at, count):
        for k in range(count):
            small[t, at + k : at + k + 1, :] = vec[:, k * LANES : (k + 1) * LANES]

    pl.semaphore_wait(bar, 10 + jnp.minimum(zp, early))
    for i in range(early):
        @pl.when(i < zp)
        def _():
            signal(tok1, pair_dev(i))

    def at_slot(s, xx, yy):
        if isinstance(s, int) and s == nc:
            return small.at[2 * xx + yy]
        return g.at[s * nt + 2 * xx + yy]

    def slots_of(s, count):
        return (small if isinstance(s, int) and s == nc else g).at[pl.ds(0, count)]

    def send(s, a, k, device):
        done = sg.at[1 if isinstance(s, int) and s == nc else 0]
        rcopy(a, a, done, rg.at[s, k], device).start()

    def arrived(s, k, count=1):
        a = slots_of(s, count)
        rcopy(a, a, sg.at[0], rg.at[s, k], partner_y).wait_recv()

    def cond(pred, work):
        if isinstance(pred, bool):
            if pred:
                work()
        else:
            pl.when(pred)(work)

    def start_y(s):
        send(s, at_slot(s, x, yh), 0, partner_y)

    def stage_own(s):
        a = at_slot(s, x, yh)
        send(s, a, 1 + 2 * (s % 2), right)
        send(s, a, 1 + 2 * ((s + 1) % 2), left)

    def stage_partner(s):
        arrived(s, 0)
        a = at_slot(s, x, yo)
        send(s, a, 3 - s % 2, right)
        send(s, a, 3 - (s + 1) % 2, left)

    def stage_far_own(s):
        arrived(s, 1)
        cond(s % 2 == 0, lambda: send(s, at_slot(s, xl, yh), 3, right))
        cond(s % 2 == 1, lambda: send(s, at_slot(s, xr, yh), 3, left))

    def stage_far_other(s):
        arrived(s, 2)
        cond(s % 2 == 0, lambda: send(s, at_slot(s, xr, yo), 3, left))
        cond(s % 2 == 1, lambda: send(s, at_slot(s, xl, yo), 3, right))

    def stage_finish(s):
        arrived(s, 3, 4)

    load_g(0).wait()
    start_y(0)
    stage_own(0)
    loads[0].wait()
    loads[1].wait()
    held = jnp.where(ow[...] == t, ah[0], jnp.float32(0.0))
    mh[...] = held
    to_rows(jnp.max(held, axis=0, keepdims=True), 0, nc)
    hcol = pl.multiple_of(zp * LANES, LANES)
    hrow = pl.multiple_of(c * 8, 8)
    small[t, 8:16, :] = mh[pl.ds(hrow, 8), pl.ds(hcol, LANES)]
    loads[3].wait()
    to_rows(jnp.max(jnp.abs(acol[...].astype(jnp.float32)), axis=0, keepdims=True), 16, nc)

    start_y(nc)
    stage_own(nc)
    rest = acol.at[:, pl.ds(0, (nc - 1) * LANES)]
    pltpu.make_async_copy(rest, rest, ld_g.at[1]).wait()
    for s in range(1, min(4, nc)):
        start_y(s)
        if s < min(3, AHEAD):
            stage_own(s)

    def p2_copy():
        return rcopy(pv, pcore, sp2, rp2, other_core)

    loads[2].wait()
    gscale = QUANT_LIMIT / jnp.maximum(jnp.max(gh[...], axis=0, keepdims=True), SCALE_FLOOR)
    pad = jnp.zeros((1, wp - width), jnp.float32)
    gcol[...] = jnp.broadcast_to(jnp.concatenate([gscale, pad], axis=1), (LANES, wp)).T
    loads[4].wait()
    loads[5].wait()
    for i in range(nt):
        at = nc * LANES + i * width

        @pl.when(t == i)
        def _():
            gsl[...] = sl[:, at : at + width]


    def quant_rows(at, count):
        scale = gcol[at, :]
        top = jnp.zeros((count, LANES), jnp.float32)
        for j in range(tokens // LANES):
            v = graw[at, j * LANES : (j + 1) * LANES].astype(jnp.float32)
            gq[at, j * LANES : (j + 1) * LANES] = jnp.clip(
                v * scale, -QUANT_LIMIT, QUANT_LIMIT
            ).astype(jnp.bfloat16)
            top = jnp.maximum(top, jnp.abs(v))
        gpk[at, :] = top

    def quant_block(i, carry):
        quant_rows(pl.ds(pl.multiple_of(i * BLOCK, BLOCK), BLOCK), BLOCK)
        return carry

    full = width // BLOCK
    for j in range(1, AHEAD):
        if j <= 3:
            lax.fori_loop((j - 1) * full // 3, j * full // 3, quant_block, 0)
        if j - 1 < nc:
            stage_partner(j - 1)
            stage_far_own(j - 1)
        if j == 1:
            stage_partner(nc)
            stage_far_own(nc)
        if j == 2:
            stage_far_other(nc)
        if 0 <= j - 2 < min(AHEAD - 3, nc):
            stage_far_other(j - 2)
        if j + 3 < min(AHEAD + 1, nc):
            start_y(j + 3)
        if j + 2 < min(AHEAD, nc):
            stage_own(j + 2)
    if width > full * BLOCK:
        quant_rows(slice(full * BLOCK, width), width - full * BLOCK)
    gq[width:, :] = jnp.zeros((wp - width, tokens), jnp.bfloat16)
    gpk[width:, :] = jnp.zeros((wp - width, LANES), jnp.float32)
    gpeak = jnp.max(gpk[...].T, axis=0, keepdims=True)

    stage_finish(nc)
    total_small = small[0]
    apeak = small[0, 16:24, :]
    for i in range(1, nt):
        total_small = total_small + small[i]
        apeak = jnp.maximum(apeak, small[i, 16:24, :])
    ascale = QUANT_LIMIT / jnp.maximum(total_small[0:8, :], SCALE_FLOOR)
    for k in range(nc):
        scales[k] = ascale[k : k + 1, :]
    hb[...] = total_small[8:16, :]
    ch[pl.ds(hrow, 8), pl.ds(hcol, LANES)] = total_small[8:16, :]
    pv[0:8, :] = apeak
    for k in range(wp // LANES):
        pv[8 + k : 9 + k, :] = gpeak[:, k * LANES : (k + 1) * LANES]
    pv[8 + wp // LANES :, :] = jnp.zeros((8 - wp // LANES, LANES), jnp.float32)
    p2_copy().start()

    def r1_copy(s):
        return rcopy(s1.at[s], r1.at[s], sr1, rr1.at[s], other_core)

    def r4_copy(s):
        return rcopy(s4.at[s], rb.at[zp], sr4, rr4, pair_dev(chunk(s)))

    def compute(s):
        scale = scales[chunk(s)]
        for i in range(nt):
            v = g[s * nt + i].astype(jnp.float32) * scale
            q[pl.ds(i * rows, rows), :] = jnp.clip(v, -QUANT_LIMIT, QUANT_LIMIT).astype(jnp.bfloat16)
        out = jnp.dot(gq[...], q[...], preferred_element_type=jnp.float32)
        part[...] = out.T.reshape(8, 16, wp)

    def start_r1(s):
        for i in range(4):
            s1[s, i] = part[2 * i + 1 - c].astype(jnp.bfloat16)
        r1_copy(s).start()

    def quad_copy(s, i):
        zz, yy, _ = cube_index(2 * i)
        return rcopy(
            s2.at[s * 3 + i - 1], r2.at[s * 3 + i - 1], sr2, rr2.at[s], dp_dev(2 * zp + zz, yy, c)
        )

    def finish_r1(s):
        r1_copy(s).wait_recv()
        for i in range(4):
            zz, yy, _ = cube_index(2 * i)
            k = 2 * zz + yy
            total = part[2 * k + c] + r1[s, k].astype(jnp.float32)
            if i == 0:
                keep2[s % 4] = total
            else:
                s2[s * 3 + i - 1] = total.astype(jnp.bfloat16)
        for i in range(1, 4):
            quad_copy(s, i).start()

    def finish_quad(s):
        total = keep2[s % 4]
        a = r2.at[pl.ds(s * 3, 3)]
        rcopy(a, a, sr2, rr2.at[s], other_core).wait_recv()
        for i in range(3):
            total = total + r2[s * 3 + i].astype(jnp.float32)
        emit(s, total)

    def emit(s, total):
        s4[s] = total.astype(jnp.bfloat16)

        @pl.when(chunk(s) == zp)
        def _():
            own_sum[...] = total

        @pl.when(chunk(s) != zp)
        def _():
            r4_copy(s).start()

    def p3_copy():
        return rcopy(pcore, pylo, sp3, rp3, other_yl)

    def p4_copy():
        return rcopy(pylo, pzz, sp4, rp4, other_z)

    def p5_copy(i):
        return rcopy(pzz, pfar.at[i], sp5, rp5, pair_dev((zp + i) % nc))

    def h3_copy(i):
        dst = ch.at[pl.ds(hrow, 8), pl.ds(hcol, LANES)]
        return rcopy(hb, dst, sh3, rh3, pair_dev((zp + i) % nc))

    def h3_all():
        a = ch.at[pl.ds(0, 8), pl.ds(0, (nc - 1) * LANES)]
        return rcopy(a, a, sh3, rh3, other_core)

    def p5_all():
        a = pfar.at[pl.ds(1, nc - 1)]
        return rcopy(a, a, sp5, rp5, other_core)

    def h4_copy():
        half = ch.at[pl.ds(hrow, 8), :]
        return rcopy(half, half, sh4, rh4, other_core)

    def h4_arrival():
        half = ch.at[pl.ds(pl.multiple_of(8 - hrow, 8), 8), :]
        return rcopy(half, half, sh4, rh4, other_core)

    def side_work(s):
        def p3():
            p2_copy().wait_recv()
            pcore[...] = jnp.maximum(pcore[...], pv[...])
            p3_copy().start()

        def p4():
            p3_copy().wait_recv()
            pylo[...] = jnp.maximum(pylo[...], pcore[...])
            p4_copy().start()

        def far():
            p4_copy().wait_recv()
            pzz[...] = jnp.maximum(pzz[...], pylo[...])
            for i in range(1, nc):
                h3_copy(i).start()
            for i in range(1, nc):
                p5_copy(i).start()

        todo = [(0, p3), (1, p4), (2, far)]
        for at, work in todo:
            pl.when(s == min(at, nc - 1))(work)

    def tokens_wait():
        @pl.when(zp < early)
        def _():
            pl.semaphore_wait(tok1, nc - 1 - zp)
            for pp in range(early, nc):
                @pl.when((nc - 1 - pp) % early == zp)
                def _():
                    signal(tok2, pair_dev(pp))

        @pl.when(zp >= early)
        def _():
            pl.semaphore_wait(tok2, 1)

    def step(s, carry):
        @pl.when(s + AHEAD + 1 < nc)
        def _():
            start_y(s + AHEAD + 1)

        @pl.when(s + AHEAD < nc)
        def _():
            stage_own(s + AHEAD)

        @pl.when(s >= 1)
        def _():
            finish_r1(s - 1)

        stage_finish(s)
        compute(s)
        start_r1(s)

        @pl.when(jnp.logical_and(s == 0, AHEAD - 3 < nc))
        def _():
            stage_far_other(s + AHEAD - 3)

        @pl.when(s + AHEAD - 1 < nc)
        def _():
            stage_partner(s + AHEAD - 1)
            stage_far_own(s + AHEAD - 1)

        @pl.when(s == tok_step)
        def _():
            tokens_wait()

        @pl.when(jnp.logical_and(s >= 2, s < nc - 1))
        def _():
            finish_quad(s - 2)

        @pl.when(s + AHEAD - 2 < nc)
        def _():
            stage_far_other(s + AHEAD - 2)

        side_work(s)
        return carry

    lax.fori_loop(0, nc, step, 0)
    last = nc - 1
    finish_r1(last)
    if nc > 2:
        finish_quad(last - 2)
    h3_all().wait_recv()
    h4_copy().start()
    if nc > 1:
        finish_quad(last - 1)
    top = pzz[...]
    p5_all().wait_recv()
    for i in range(1, nc):
        top = jnp.maximum(top, pfar[i])
    for k in range(nc):
        peak_row[:, k * LANES : (k + 1) * LANES] = top[k : k + 1, :]
    for k in range(wp // LANES):
        n = min(width - k * LANES, LANES)
        gpeak_row[:, k * LANES : k * LANES + n] = top[8 + k : 9 + k, :n]
    hist_row = lax.broadcasted_iota(jnp.int32, ghist_out.shape, 0)
    ghist_out[...] = jnp.where(hist_row == gsl[...], gpeak_row[...], gh[...])
    h4_arrival().wait_recv()
    hist_row = lax.broadcasted_iota(jnp.int32, hist_out.shape, 0)
    hist_out[...] = jnp.where(hist_row == sl[:, : nc * LANES], peak_row[...], ch[...])
    lane = lax.broadcasted_iota(jnp.int32, (16, LANES), 1)
    row = lax.broadcasted_iota(jnp.int32, (16, LANES), 0)
    mine = lane == row + (zq * 4 + yl * 2 + c) * 16
    row_scale = jnp.sum(jnp.where(mine, scales[zp], jnp.float32(0.0)), axis=1, keepdims=True)
    gscale = QUANT_LIMIT / jnp.maximum(jnp.max(gh[...], axis=0, keepdims=True), SCALE_FLOOR)
    finish_quad(last)

    total = own_sum[...]
    a = rb.at[pl.ds(0, nc - 1)]
    rcopy(a, a, sr4, rr4, other_core).wait_recv()
    for i in range(1, nc):
        frm = (zp + i) % nc
        total = total + rb[frm].astype(jnp.float32)
    wgrad_out[...] = total[:, :width] / (row_scale * gscale) * factor

    for a, done in (
        (g.at[pl.ds(0, 7 * nc)], sg.at[0]),
        (small.at[pl.ds(0, 7)], sg.at[1]),
        (s1, sr1),
        (s2, sr2),
        (s4.at[pl.ds(0, nc - 1)], sr4),
    ):
        rcopy(a, a, done, rr4, other_core).wait_send()
    h4_copy().wait_send()
    p2_copy().wait_send()
    p3_copy().wait_send()
    p4_copy().wait_send()
    h3_all().wait_send()
    p5_all().wait_send()


def fused(acts, grads, ahist, ghist, owner, slots, nz, nx, factor):
    rows, model = acts.shape
    width, tokens = grads.shape
    nc, nt = nz // 2, 2 * nx
    wp = -(-width // LANES) * LANES
    f32, bf16 = jnp.float32, jnp.bfloat16
    dma = pltpu.SemaphoreType.DMA
    vm = pltpu.VMEM
    scratch = [
        vm((nc * nt, rows, LANES), bf16),
        vm((rows, model), bf16),
        vm((width, tokens), bf16),
        vm((wp, tokens), bf16),
        vm((tokens, LANES), bf16),
        vm((1, 16, model), f32),
        vm((16, width), f32),
        vm((1, model), jnp.int32),
        vm((1, slots.shape[0]), jnp.int32),
        vm((1, width), jnp.int32),
        vm((1, model), f32),
        vm((1, width), f32),
        vm((wp, LANES), f32),
        vm((wp, LANES), f32),
        vm((nc, 1, LANES), f32),
        vm((16, model), f32),
        vm((nt, 24, LANES), f32),
        vm((8, LANES), f32),
        vm((16, model), f32),
        vm((16, LANES), f32),
        vm((16, LANES), f32),
        vm((16, LANES), f32),
        vm((16, LANES), f32),
        vm((nc, 16, LANES), f32),
        vm((8, 16, wp), f32),
        vm((nc, 4, 16, wp), bf16),
        vm((nc, 4, 16, wp), bf16),
        vm((nc * 3, 16, wp), bf16),
        vm((nc * 3, 16, wp), bf16),
        vm((4, 16, wp), f32),
        vm((nc, 16, wp), bf16),
        vm((nc, 16, wp), bf16),
        vm((16, wp), f32),
        dma((2,)), dma((6,)),
        dma((2,)), dma((nc + 1, 4)),
        dma, dma, dma, dma,
        dma, dma, dma, dma, dma, dma, dma, dma,
        dma, dma((nc,)), dma, dma((nc,)), dma, dma,
        pltpu.SemaphoreType.REGULAR, pltpu.SemaphoreType.REGULAR,
    ]
    vspec = pl.BlockSpec(memory_space=pltpu.VMEM)
    anyspec = pl.BlockSpec(memory_space=pl.ANY)
    return pl.pallas_call(
        functools.partial(kernel, nz, nx, factor),
        out_shape=[
            jax.ShapeDtypeStruct((16, width), f32),
            jax.ShapeDtypeStruct((16, model), f32),
            jax.ShapeDtypeStruct((16, width), f32),
        ],
        in_specs=[anyspec] * 6,
        out_specs=[vspec] * 3,
        scratch_shapes=scratch,
        compiler_params=pltpu.CompilerParams(
            collective_id=0, has_side_effects=True, vmem_limit_bytes=55100 * 1024
        ),
    )(acts, grads, ahist, ghist, owner, slots)


def body(nz, nx, activations, gradients, act_history, grad_history, owner_rank, history_slot):
    factor = 1.0 / math.sqrt(gradients.shape[0] * lax.axis_size("dp"))
    weight_grad, act_history_out, grad_history_out = fused(
        activations, gradients.T, act_history, grad_history,
        owner_rank.reshape(1, -1), history_slot, nz, nx, factor,
    )
    return (weight_grad, act_history_out[None], grad_history_out)


def solution(mesh):
    nz = mesh.shape["dp"] // 4
    nx = mesh.shape["tensor"] // 2
    placed = (
        P(("dp", "tensor"), None),
        P("dp", "tensor"),
        P("tensor", None, None),
        P(None, "tensor"),
        P(),
        P(),
    )
    return jax.shard_map(
        functools.partial(body, nz, nx),
        mesh=mesh,
        in_specs=placed,
        out_specs=(P("dp", "tensor"), P("tensor", None, None), P(None, "tensor")),
        check_vma=False,
    )
```

```python
import functools
import math

import jax
import jax.numpy as jnp
from jax import lax
from jax.experimental import pallas as pl
from jax.experimental.pallas import tpu as pltpu
from jax.sharding import PartitionSpec as P

QUANT_LIMIT = 448.0
SCALE_FLOOR = 0.25
LANES = 128
BLOCK = 64
AHEAD = 4
MESH = pl.DeviceIdType.MESH


def kernel(
    nz, nx, acts, grads, ahist, ghist, owner, slots,
    pack_out, hist_out,
    g, acol, graw, gq, q, ah, gh, ow, sl, gsl, peak_row, gpeak_row, gcol, gpk, scales, mh, small, hb, ch,
    pv, pcore, pylo, pzz, pfar,
    part, s1, r1, s2, r2, keep2, s4, rb, own_sum,
    ld_g, ld_x,
    sg, rg,
    sh3, rh3, sh4, rh4, sp2, rp2, sp3, rp3, sp4, rp4, sp5, rp5,
    sr1, rr1, sr2, rr2, sr4, rr4, tok1, tok2,
):
    nc = nz // 2
    nt = 2 * nx
    early = max(3 * nc // 8, 1)
    tok_step = min(1, nc - 1)
    rows = acts.shape[0]
    width, tokens = grads.shape
    wp = gq.shape[0]
    t = lax.axis_index("tensor")
    dpi = lax.axis_index("dp")
    x, yh = t // 2, t % 2
    z, yl, c = dpi // 4, (dpi // 2) % 2, dpi % 2
    zp, zq = z // 2, z % 2
    xr, xl, xf = (x + 1) % nx, (x + nx - 1) % nx, (x + 2) % nx
    yo = 1 - yh

    def tensor_dev(tt):
        return {"dp": dpi, "tensor": tt}

    def dp_dev(zz, yy, cc):
        return {"dp": zz * 4 + yy * 2 + cc, "tensor": t}

    def pair_dev(pp):
        return dp_dev(2 * pp + zq, yl, c)

    def rcopy(src, dst, ss, rs, device):
        return pltpu.make_async_remote_copy(
            src_ref=src, dst_ref=dst, send_sem=ss, recv_sem=rs,
            device_id=device, device_id_type=MESH,
        )

    def signal(sem, device):
        pl.semaphore_signal(sem, inc=1, device_id=device, device_id_type=MESH)

    def chunk(s):
        hf = nc // 2
        late = s // hf
        j = 2 * hf - 1 - s
        high = zp // hf
        u = high * (zp - hf) + (1 - high) * (hf - 1 - zp)
        flip = (u + j) % 2 + 2 * ((u // 2 + j // 2) % 2)
        return (1 - late) * s + late * (hf + flip % hf)

    partner_y = tensor_dev(2 * x + yo)
    right = tensor_dev(2 * xr + yh)
    left = tensor_dev(2 * xl + yh)
    other_core = dp_dev(z, yl, 1 - c)
    other_yl = dp_dev(z, 1 - yl, c)
    other_z = dp_dev(2 * zp + 1 - zq, yl, c)

    def cube_index(i):
        return (zq + i // 4) % 2, (yl + i // 2 % 2) % 2, (c + i % 2) % 2

    def cube_dev(i):
        zz, yy, cc = cube_index(i)
        return dp_dev(2 * zp + zz, yy, cc)

    def load_g(s):
        col = pl.multiple_of(chunk(s) * LANES, LANES)
        return pltpu.make_async_copy(
            acts.at[:, pl.ds(col, LANES)], g.at[s * nt + t], ld_g.at[min(s, 1)]
        )

    loads = [
        pltpu.make_async_copy(src, dst, ld_x.at[i])
        for i, (src, dst) in enumerate(
            [(ahist, ah), (owner, ow), (ghist, gh), (acts, acol), (grads, graw), (slots, sl.at[0])]
        )
    ]
    bar = pltpu.get_barrier_semaphore()
    for device in (partner_y, right, left):
        signal(bar, device)
    for i in range(1, 8):
        signal(bar, cube_dev(i))
    for i in range(1, nc):
        @pl.when(jnp.logical_and(zp < early, zp + i < nc))
        def _():
            signal(bar, pair_dev(zp + i))

    load_g(0).start()
    for i in (0, 1, 3):
        loads[i].start()
    for s in range(1, nc):
        load_g(s).start()
    for i in (2, 4, 5):
        loads[i].start()

    def to_rows(vec, at, count):
        for k in range(count):
            small[t, at + k : at + k + 1, :] = vec[:, k * LANES : (k + 1) * LANES]

    pl.semaphore_wait(bar, 10 + jnp.minimum(zp, early))
    for i in range(early):
        @pl.when(i < zp)
        def _():
            signal(tok1, pair_dev(i))

    def at_slot(s, xx, yy):
        if isinstance(s, int) and s == nc:
            return small.at[2 * xx + yy]
        return g.at[s * nt + 2 * xx + yy]

    def slots_of(s, count):
        return (small if isinstance(s, int) and s == nc else g).at[pl.ds(0, count)]

    def send(s, a, k, device):
        done = sg.at[1 if isinstance(s, int) and s == nc else 0]
        rcopy(a, a, done, rg.at[s, k], device).start()

    def arrived(s, k, count=1):
        a = slots_of(s, count)
        rcopy(a, a, sg.at[0], rg.at[s, k], partner_y).wait_recv()

    def cond(pred, work):
        if isinstance(pred, bool):
            if pred:
                work()
        else:
            pl.when(pred)(work)

    def start_y(s):
        send(s, at_slot(s, x, yh), 0, partner_y)

    def stage_own(s):
        a = at_slot(s, x, yh)
        send(s, a, 1 + 2 * (s % 2), right)
        send(s, a, 1 + 2 * ((s + 1) % 2), left)

    def stage_partner(s):
        arrived(s, 0)
        a = at_slot(s, x, yo)
        send(s, a, 3 - s % 2, right)
        send(s, a, 3 - (s + 1) % 2, left)

    def stage_far_own(s):
        arrived(s, 1)
        cond(s % 2 == 0, lambda: send(s, at_slot(s, xl, yh), 3, right))
        cond(s % 2 == 1, lambda: send(s, at_slot(s, xr, yh), 3, left))

    def stage_far_other(s):
        arrived(s, 2)
        cond(s % 2 == 0, lambda: send(s, at_slot(s, xr, yo), 3, left))
        cond(s % 2 == 1, lambda: send(s, at_slot(s, xl, yo), 3, right))

    def stage_finish(s):
        arrived(s, 3, 4)

    load_g(0).wait()
    start_y(0)
    stage_own(0)
    loads[0].wait()
    loads[1].wait()
    held = jnp.where(ow[...] == t, ah[0], jnp.float32(0.0))
    mh[...] = held
    to_rows(jnp.max(held, axis=0, keepdims=True), 0, nc)
    hcol = pl.multiple_of(zp * LANES, LANES)
    hrow = pl.multiple_of(c * 8, 8)
    small[t, 8:16, :] = mh[pl.ds(hrow, 8), pl.ds(hcol, LANES)]
    loads[3].wait()
    to_rows(jnp.max(jnp.abs(acol[...].astype(jnp.float32)), axis=0, keepdims=True), 16, nc)

    start_y(nc)
    stage_own(nc)
    rest = acol.at[:, pl.ds(0, (nc - 1) * LANES)]
    pltpu.make_async_copy(rest, rest, ld_g.at[1]).wait()
    for s in range(1, min(4, nc)):
        start_y(s)
        if s < min(3, AHEAD):
            stage_own(s)

    def p2_copy():
        return rcopy(pv, pcore, sp2, rp2, other_core)

    loads[2].wait()
    gscale = QUANT_LIMIT / jnp.maximum(jnp.max(gh[...], axis=0, keepdims=True), SCALE_FLOOR)
    pad = jnp.zeros((1, wp - width), jnp.float32)
    gcol[...] = jnp.broadcast_to(jnp.concatenate([gscale, pad], axis=1), (LANES, wp)).T
    loads[4].wait()
    loads[5].wait()
    for i in range(nt):
        at = nc * LANES + i * width

        @pl.when(t == i)
        def _():
            gsl[...] = sl[:, at : at + width]


    def quant_rows(at, count):
        scale = gcol[at, :]
        top = jnp.zeros((count, LANES), jnp.float32)
        for j in range(tokens // LANES):
            v = graw[at, j * LANES : (j + 1) * LANES].astype(jnp.float32)
            gq[at, j * LANES : (j + 1) * LANES] = jnp.clip(
                v * scale, -QUANT_LIMIT, QUANT_LIMIT
            ).astype(jnp.bfloat16)
            top = jnp.maximum(top, jnp.abs(v))
        gpk[at, :] = top

    def quant_block(i, carry):
        quant_rows(pl.ds(pl.multiple_of(i * BLOCK, BLOCK), BLOCK), BLOCK)
        return carry

    full = width // BLOCK
    for j in range(1, AHEAD):
        if j <= 3:
            lax.fori_loop((j - 1) * full // 3, j * full // 3, quant_block, 0)
        if j - 1 < nc:
            stage_partner(j - 1)
            stage_far_own(j - 1)
        if j == 1:
            stage_partner(nc)
            stage_far_own(nc)
        if j == 2:
            stage_far_other(nc)
        if 0 <= j - 2 < min(AHEAD - 3, nc):
            stage_far_other(j - 2)
        if j + 3 < min(AHEAD + 1, nc):
            start_y(j + 3)
        if j + 2 < min(AHEAD, nc):
            stage_own(j + 2)
    if width > full * BLOCK:
        quant_rows(slice(full * BLOCK, width), width - full * BLOCK)
    gq[width:, :] = jnp.zeros((wp - width, tokens), jnp.bfloat16)
    gpk[width:, :] = jnp.zeros((wp - width, LANES), jnp.float32)
    gpeak = jnp.max(gpk[...].T, axis=0, keepdims=True)

    stage_finish(nc)
    total_small = small[0]
    apeak = small[0, 16:24, :]
    for i in range(1, nt):
        total_small = total_small + small[i]
        apeak = jnp.maximum(apeak, small[i, 16:24, :])
    ascale = QUANT_LIMIT / jnp.maximum(total_small[0:8, :], SCALE_FLOOR)
    for k in range(nc):
        scales[k] = ascale[k : k + 1, :]
    hb[...] = total_small[8:16, :]
    ch[pl.ds(hrow, 8), pl.ds(hcol, LANES)] = total_small[8:16, :]
    pv[0:8, :] = apeak
    for k in range(wp // LANES):
        pv[8 + k : 9 + k, :] = gpeak[:, k * LANES : (k + 1) * LANES]
    pv[8 + wp // LANES :, :] = jnp.zeros((8 - wp // LANES, LANES), jnp.float32)
    p2_copy().start()

    def r1_copy(s):
        return rcopy(s1.at[s], r1.at[s], sr1, rr1.at[s], other_core)

    def r4_copy(s):
        return rcopy(s4.at[s], rb.at[zp], sr4, rr4, pair_dev(chunk(s)))

    def compute(s):
        scale = scales[chunk(s)]
        for i in range(nt):
            v = g[s * nt + i].astype(jnp.float32) * scale
            q[pl.ds(i * rows, rows), :] = jnp.clip(v, -QUANT_LIMIT, QUANT_LIMIT).astype(jnp.bfloat16)
        out = jnp.dot(gq[...], q[...], preferred_element_type=jnp.float32)
        part[...] = out.T.reshape(8, 16, wp)

    def start_r1(s):
        for i in range(4):
            s1[s, i] = part[2 * i + 1 - c].astype(jnp.bfloat16)
        r1_copy(s).start()

    def quad_copy(s, i):
        zz, yy, _ = cube_index(2 * i)
        return rcopy(
            s2.at[s * 3 + i - 1], r2.at[s * 3 + i - 1], sr2, rr2.at[s], dp_dev(2 * zp + zz, yy, c)
        )

    def finish_r1(s):
        r1_copy(s).wait_recv()
        for i in range(4):
            zz, yy, _ = cube_index(2 * i)
            k = 2 * zz + yy
            total = part[2 * k + c] + r1[s, k].astype(jnp.float32)
            if i == 0:
                keep2[s % 4] = total
            else:
                s2[s * 3 + i - 1] = total.astype(jnp.bfloat16)
        for i in range(1, 4):
            quad_copy(s, i).start()

    def finish_quad(s):
        total = keep2[s % 4]
        a = r2.at[pl.ds(s * 3, 3)]
        rcopy(a, a, sr2, rr2.at[s], other_core).wait_recv()
        for i in range(3):
            total = total + r2[s * 3 + i].astype(jnp.float32)
        emit(s, total)

    def emit(s, total):
        s4[s] = total.astype(jnp.bfloat16)

        @pl.when(chunk(s) == zp)
        def _():
            own_sum[...] = total

        @pl.when(chunk(s) != zp)
        def _():
            r4_copy(s).start()

    def p3_copy():
        return rcopy(pcore, pylo, sp3, rp3, other_yl)

    def p4_copy():
        return rcopy(pylo, pzz, sp4, rp4, other_z)

    def p5_copy(i):
        return rcopy(pzz, pfar.at[i], sp5, rp5, pair_dev((zp + i) % nc))

    def h3_copy(i):
        dst = ch.at[pl.ds(hrow, 8), pl.ds(hcol, LANES)]
        return rcopy(hb, dst, sh3, rh3, pair_dev((zp + i) % nc))

    def h3_all():
        a = ch.at[pl.ds(0, 8), pl.ds(0, (nc - 1) * LANES)]
        return rcopy(a, a, sh3, rh3, other_core)

    def p5_all():
        a = pfar.at[pl.ds(1, nc - 1)]
        return rcopy(a, a, sp5, rp5, other_core)

    def h4_copy():
        half = ch.at[pl.ds(hrow, 8), :]
        return rcopy(half, half, sh4, rh4, other_core)

    def h4_arrival():
        half = ch.at[pl.ds(pl.multiple_of(8 - hrow, 8), 8), :]
        return rcopy(half, half, sh4, rh4, other_core)

    def side_work(s):
        def p3():
            p2_copy().wait_recv()
            pcore[...] = jnp.maximum(pcore[...], pv[...])
            p3_copy().start()

        def p4():
            p3_copy().wait_recv()
            pylo[...] = jnp.maximum(pylo[...], pcore[...])
            p4_copy().start()

        def far():
            p4_copy().wait_recv()
            pzz[...] = jnp.maximum(pzz[...], pylo[...])
            for i in range(1, nc):
                h3_copy(i).start()
            for i in range(1, nc):
                p5_copy(i).start()

        todo = [(0, p3), (1, p4), (2, far)]
        for at, work in todo:
            pl.when(s == min(at, nc - 1))(work)

    def tokens_wait():
        @pl.when(zp < early)
        def _():
            pl.semaphore_wait(tok1, nc - 1 - zp)
            for pp in range(early, nc):
                @pl.when((nc - 1 - pp) % early == zp)
                def _():
                    signal(tok2, pair_dev(pp))

        @pl.when(zp >= early)
        def _():
            pl.semaphore_wait(tok2, 1)

    def step(s, carry):
        @pl.when(s + AHEAD + 1 < nc)
        def _():
            start_y(s + AHEAD + 1)

        @pl.when(s + AHEAD < nc)
        def _():
            stage_own(s + AHEAD)

        @pl.when(s >= 1)
        def _():
            finish_r1(s - 1)

        stage_finish(s)
        compute(s)
        start_r1(s)

        @pl.when(jnp.logical_and(s == 0, AHEAD - 3 < nc))
        def _():
            stage_far_other(s + AHEAD - 3)

        @pl.when(s + AHEAD - 1 < nc)
        def _():
            stage_partner(s + AHEAD - 1)
            stage_far_own(s + AHEAD - 1)

        @pl.when(s == tok_step)
        def _():
            tokens_wait()

        @pl.when(jnp.logical_and(s >= 2, s < nc - 1))
        def _():
            finish_quad(s - 2)

        @pl.when(s + AHEAD - 2 < nc)
        def _():
            stage_far_other(s + AHEAD - 2)

        side_work(s)
        return carry

    lax.fori_loop(0, nc, step, 0)
    last = nc - 1
    finish_r1(last)
    if nc > 2:
        finish_quad(last - 2)
    h3_all().wait_recv()
    h4_copy().start()
    if nc > 1:
        finish_quad(last - 1)
    top = pzz[...]
    p5_all().wait_recv()
    for i in range(1, nc):
        top = jnp.maximum(top, pfar[i])
    for k in range(nc):
        peak_row[:, k * LANES : (k + 1) * LANES] = top[k : k + 1, :]
    for k in range(wp // LANES):
        n = min(width - k * LANES, LANES)
        gpeak_row[:, k * LANES : k * LANES + n] = top[8 + k : 9 + k, :n]
    hist_row = lax.broadcasted_iota(jnp.int32, (16, width), 0)
    pack_out[16:32, :] = jnp.where(hist_row == gsl[...], gpeak_row[...], gh[...])
    h4_arrival().wait_recv()
    hist_row = lax.broadcasted_iota(jnp.int32, hist_out.shape, 0)
    hist_out[...] = jnp.where(hist_row == sl[:, : nc * LANES], peak_row[...], ch[...])
    lane = lax.broadcasted_iota(jnp.int32, (16, LANES), 1)
    row = lax.broadcasted_iota(jnp.int32, (16, LANES), 0)
    mine = lane == row + (zq * 4 + yl * 2 + c) * 16
    row_scale = jnp.sum(jnp.where(mine, scales[zp], jnp.float32(0.0)), axis=1, keepdims=True)
    gscale = QUANT_LIMIT / jnp.maximum(jnp.max(gh[...], axis=0, keepdims=True), SCALE_FLOOR)
    finish_quad(last)

    total = own_sum[...]
    a = rb.at[pl.ds(0, nc - 1)]
    rcopy(a, a, sr4, rr4, other_core).wait_recv()
    for i in range(1, nc):
        frm = (zp + i) % nc
        total = total + rb[frm].astype(jnp.float32)
    pack_out[0:16, :] = total[:, :width] / (row_scale * gscale)

    for a, done in (
        (g.at[pl.ds(0, 7 * nc)], sg.at[0]),
        (small.at[pl.ds(0, 7)], sg.at[1]),
        (s1, sr1),
        (s2, sr2),
        (s4.at[pl.ds(0, nc - 1)], sr4),
    ):
        rcopy(a, a, done, rr4, other_core).wait_send()
    h4_copy().wait_send()
    p2_copy().wait_send()
    p3_copy().wait_send()
    p4_copy().wait_send()
    h3_all().wait_send()
    p5_all().wait_send()


def fused(acts, grads, ahist, ghist, owner, slots, nz, nx):
    rows, model = acts.shape
    width, tokens = grads.shape
    nc, nt = nz // 2, 2 * nx
    wp = -(-width // LANES) * LANES
    f32, bf16 = jnp.float32, jnp.bfloat16
    dma = pltpu.SemaphoreType.DMA
    vm = pltpu.VMEM
    scratch = [
        vm((nc * nt, rows, LANES), bf16),
        vm((rows, model), bf16),
        vm((width, tokens), bf16),
        vm((wp, tokens), bf16),
        vm((tokens, LANES), bf16),
        vm((1, 16, model), f32),
        vm((16, width), f32),
        vm((1, model), jnp.int32),
        vm((1, slots.shape[0]), jnp.int32),
        vm((1, width), jnp.int32),
        vm((1, model), f32),
        vm((1, width), f32),
        vm((wp, LANES), f32),
        vm((wp, LANES), f32),
        vm((nc, 1, LANES), f32),
        vm((16, model), f32),
        vm((nt, 24, LANES), f32),
        vm((8, LANES), f32),
        vm((16, model), f32),
        vm((16, LANES), f32),
        vm((16, LANES), f32),
        vm((16, LANES), f32),
        vm((16, LANES), f32),
        vm((nc, 16, LANES), f32),
        vm((8, 16, wp), f32),
        vm((nc, 4, 16, wp), bf16),
        vm((nc, 4, 16, wp), bf16),
        vm((nc * 3, 16, wp), bf16),
        vm((nc * 3, 16, wp), bf16),
        vm((4, 16, wp), f32),
        vm((nc, 16, wp), bf16),
        vm((nc, 16, wp), bf16),
        vm((16, wp), f32),
        dma((2,)), dma((6,)),
        dma((2,)), dma((nc + 1, 4)),
        dma, dma, dma, dma,
        dma, dma, dma, dma, dma, dma, dma, dma,
        dma, dma((nc,)), dma, dma((nc,)), dma, dma,
        pltpu.SemaphoreType.REGULAR, pltpu.SemaphoreType.REGULAR,
    ]
    vspec = pl.BlockSpec(memory_space=pltpu.VMEM)
    anyspec = pl.BlockSpec(memory_space=pl.ANY)
    return pl.pallas_call(
        functools.partial(kernel, nz, nx),
        out_shape=[
            jax.ShapeDtypeStruct((32, width), f32),
            jax.ShapeDtypeStruct((16, model), f32),
        ],
        in_specs=[anyspec] * 6,
        out_specs=[vspec] * 2,
        scratch_shapes=scratch,
        compiler_params=pltpu.CompilerParams(
            collective_id=0, has_side_effects=True, vmem_limit_bytes=60 * 1024 * 1024
        ),
    )(acts, grads, ahist, ghist, owner, slots)


def body(nz, nx, activations, gradients, act_history, grad_history, owner_rank, history_slot):
    factor = 1.0 / math.sqrt(gradients.shape[0] * lax.axis_size("dp"))
    packed, act_history_out = fused(
        activations, gradients.T, act_history, grad_history,
        owner_rank.reshape(1, -1), history_slot, nz, nx,
    )
    return (packed[:16] * factor, jnp.abs(act_history_out)[None], jnp.abs(packed[16:]))


def solution(mesh):
    nz = mesh.shape["dp"] // 4
    nx = mesh.shape["tensor"] // 2
    placed = (
        P(("dp", "tensor"), None),
        P("dp", "tensor"),
        P("tensor", None, None),
        P(None, "tensor"),
        P(),
        P(),
    )
    return jax.shard_map(
        functools.partial(body, nz, nx),
        mesh=mesh,
        in_specs=placed,
        out_specs=(P("dp", "tensor"), P("tensor", None, None), P(None, "tensor")),
        check_vma=False,
    )
```

```python
import functools
import math

import jax
import jax.numpy as jnp
from jax import lax
from jax.experimental import pallas as pl
from jax.experimental.pallas import tpu as pltpu
from jax.sharding import PartitionSpec as P

QUANT_LIMIT = 448.0
SCALE_FLOOR = 0.25
LANES = 128
BLOCK = 64
AHEAD = 4
MESH = pl.DeviceIdType.MESH


def kernel(
    nz, nx, acts, grads, ahist, ghist, owner, slots,
    pack_out, hist_out,
    g, acol, graw, gq, q, ah, gh, ow, sl, gsl, peak_row, gpeak_row, gcol, gpk, scales, mh, small, hb, ch,
    pv, pcore, pylo, pzz, pfar,
    part, s1, r1, s2, r2, keep2, s4, rb, own_sum,
    ld_g, ld_x,
    sg, rg,
    sh3, rh3, sh4, rh4, sp2, rp2, sp3, rp3, sp4, rp4, sp5, rp5,
    sr1, rr1, sr2, rr2, sr4, rr4, tok1, tok2,
):
    nc = nz // 2
    nt = 2 * nx
    early = max(3 * nc // 8, 1)
    tok_step = min(1, nc - 1)
    rows = acts.shape[0]
    width, tokens = grads.shape
    wp = gq.shape[0]
    t = lax.axis_index("tensor")
    dpi = lax.axis_index("dp")
    x, yh = t // 2, t % 2
    z, yl, c = dpi // 4, (dpi // 2) % 2, dpi % 2
    zp, zq = z // 2, z % 2
    xr, xl, xf = (x + 1) % nx, (x + nx - 1) % nx, (x + 2) % nx
    yo = 1 - yh

    def tensor_dev(tt):
        return {"dp": dpi, "tensor": tt}

    def dp_dev(zz, yy, cc):
        return {"dp": zz * 4 + yy * 2 + cc, "tensor": t}

    def pair_dev(pp):
        return dp_dev(2 * pp + zq, yl, c)

    def rcopy(src, dst, ss, rs, device):
        return pltpu.make_async_remote_copy(
            src_ref=src, dst_ref=dst, send_sem=ss, recv_sem=rs,
            device_id=device, device_id_type=MESH,
        )

    def signal(sem, device):
        pl.semaphore_signal(sem, inc=1, device_id=device, device_id_type=MESH)

    def chunk(s):
        hf = nc // 2
        late = s // hf
        j = 2 * hf - 1 - s
        high = zp // hf
        u = high * (zp - hf) + (1 - high) * (hf - 1 - zp)
        flip = (u + j) % 2 + 2 * ((u // 2 + j // 2) % 2)
        return (1 - late) * s + late * (hf + flip % hf)

    partner_y = tensor_dev(2 * x + yo)
    right = tensor_dev(2 * xr + yh)
    left = tensor_dev(2 * xl + yh)
    other_core = dp_dev(z, yl, 1 - c)
    other_yl = dp_dev(z, 1 - yl, c)
    other_z = dp_dev(2 * zp + 1 - zq, yl, c)

    def cube_index(i):
        return (zq + i // 4) % 2, (yl + i // 2 % 2) % 2, (c + i % 2) % 2

    def cube_dev(i):
        zz, yy, cc = cube_index(i)
        return dp_dev(2 * zp + zz, yy, cc)

    def load_g(s):
        col = pl.multiple_of(chunk(s) * LANES, LANES)
        return pltpu.make_async_copy(
            acts.at[:, pl.ds(col, LANES)], g.at[s * nt + t], ld_g.at[min(s, 1)]
        )

    loads = [
        pltpu.make_async_copy(src, dst, ld_x.at[i])
        for i, (src, dst) in enumerate(
            [(ahist, ah), (owner, ow), (ghist, gh), (acts, acol), (grads, graw), (slots, sl.at[0])]
        )
    ]
    bar = pltpu.get_barrier_semaphore()
    for device in (partner_y, right, left):
        signal(bar, device)
    for i in range(1, 8):
        signal(bar, cube_dev(i))
    for i in range(1, nc):
        @pl.when(jnp.logical_and(zp < early, zp + i < nc))
        def _():
            signal(bar, pair_dev(zp + i))

    load_g(0).start()
    for i in (0, 1, 3):
        loads[i].start()
    for s in range(1, nc):
        load_g(s).start()
    for i in (2, 4, 5):
        loads[i].start()

    def to_rows(vec, at, count):
        for k in range(count):
            small[t, at + k : at + k + 1, :] = vec[:, k * LANES : (k + 1) * LANES]

    pl.semaphore_wait(bar, 10 + jnp.minimum(zp, early))
    for i in range(early):
        @pl.when(i < zp)
        def _():
            signal(tok1, pair_dev(i))

    def at_slot(s, xx, yy):
        if isinstance(s, int) and s == nc:
            return small.at[2 * xx + yy]
        return g.at[s * nt + 2 * xx + yy]

    def slots_of(s, count):
        return (small if isinstance(s, int) and s == nc else g).at[pl.ds(0, count)]

    def send(s, a, k, device):
        done = sg.at[1 if isinstance(s, int) and s == nc else 0]
        rcopy(a, a, done, rg.at[s, k], device).start()

    def arrived(s, k, count=1):
        a = slots_of(s, count)
        rcopy(a, a, sg.at[0], rg.at[s, k], partner_y).wait_recv()

    def cond(pred, work):
        if isinstance(pred, bool):
            if pred:
                work()
        else:
            pl.when(pred)(work)

    def start_y(s):
        send(s, at_slot(s, x, yh), 0, partner_y)

    def stage_own(s):
        a = at_slot(s, x, yh)
        send(s, a, 1 + 2 * (s % 2), right)
        send(s, a, 1 + 2 * ((s + 1) % 2), left)

    def stage_partner(s):
        arrived(s, 0)
        a = at_slot(s, x, yo)
        send(s, a, 3 - s % 2, right)
        send(s, a, 3 - (s + 1) % 2, left)

    def stage_far_own(s):
        arrived(s, 1)
        cond(s % 2 == 0, lambda: send(s, at_slot(s, xl, yh), 3, right))
        cond(s % 2 == 1, lambda: send(s, at_slot(s, xr, yh), 3, left))

    def stage_far_other(s):
        arrived(s, 2)
        cond(s % 2 == 0, lambda: send(s, at_slot(s, xr, yo), 3, left))
        cond(s % 2 == 1, lambda: send(s, at_slot(s, xl, yo), 3, right))

    def stage_finish(s):
        arrived(s, 3, 4)

    load_g(0).wait()
    start_y(0)
    stage_own(0)
    loads[0].wait()
    loads[1].wait()
    held = jnp.where(ow[...] == t, ah[0], jnp.float32(0.0))
    mh[...] = held
    to_rows(jnp.max(held, axis=0, keepdims=True), 0, nc)
    hcol = pl.multiple_of(zp * LANES, LANES)
    hrow = pl.multiple_of(c * 8, 8)
    small[t, 8:16, :] = mh[pl.ds(hrow, 8), pl.ds(hcol, LANES)]
    loads[3].wait()
    to_rows(jnp.max(jnp.abs(acol[...].astype(jnp.float32)), axis=0, keepdims=True), 16, nc)

    start_y(nc)
    stage_own(nc)
    rest = acol.at[:, pl.ds(0, (nc - 1) * LANES)]
    pltpu.make_async_copy(rest, rest, ld_g.at[1]).wait()
    for s in range(1, min(4, nc)):
        start_y(s)
        if s < min(3, AHEAD):
            stage_own(s)

    def p2_copy():
        return rcopy(pv, pcore, sp2, rp2, other_core)

    loads[2].wait()
    gscale = QUANT_LIMIT / jnp.maximum(jnp.max(gh[...], axis=0, keepdims=True), SCALE_FLOOR)
    pad = jnp.zeros((1, wp - width), jnp.float32)
    gcol[...] = jnp.broadcast_to(jnp.concatenate([gscale, pad], axis=1), (LANES, wp)).T
    loads[4].wait()
    loads[5].wait()
    for i in range(nt):
        at = nc * LANES + i * width

        @pl.when(t == i)
        def _():
            gsl[...] = sl[:, at : at + width]


    def quant_rows(at, count):
        scale = gcol[at, :]
        top = jnp.zeros((count, LANES), jnp.float32)
        for j in range(tokens // LANES):
            v = graw[at, j * LANES : (j + 1) * LANES].astype(jnp.float32)
            gq[at, j * LANES : (j + 1) * LANES] = jnp.clip(
                v * scale, -QUANT_LIMIT, QUANT_LIMIT
            ).astype(jnp.bfloat16)
            top = jnp.maximum(top, jnp.abs(v))
        gpk[at, :] = top

    def quant_block(i, carry):
        quant_rows(pl.ds(pl.multiple_of(i * BLOCK, BLOCK), BLOCK), BLOCK)
        return carry

    full = width // BLOCK
    for j in range(1, AHEAD):
        if j <= 3:
            lax.fori_loop((j - 1) * full // 3, j * full // 3, quant_block, 0)
        if j - 1 < nc:
            stage_partner(j - 1)
            stage_far_own(j - 1)
        if j == 1:
            stage_partner(nc)
            stage_far_own(nc)
        if j == 2:
            stage_far_other(nc)
        if 0 <= j - 2 < min(AHEAD - 3, nc):
            stage_far_other(j - 2)
        if j + 3 < min(AHEAD + 1, nc):
            start_y(j + 3)
        if j + 2 < min(AHEAD, nc):
            stage_own(j + 2)
    if width > full * BLOCK:
        quant_rows(slice(full * BLOCK, width), width - full * BLOCK)
    gq[width:, :] = jnp.zeros((wp - width, tokens), jnp.bfloat16)
    gpk[width:, :] = jnp.zeros((wp - width, LANES), jnp.float32)
    gpeak = jnp.max(gpk[...].T, axis=0, keepdims=True)

    stage_finish(nc)
    total_small = small[0]
    apeak = small[0, 16:24, :]
    for i in range(1, nt):
        total_small = total_small + small[i]
        apeak = jnp.maximum(apeak, small[i, 16:24, :])
    ascale = QUANT_LIMIT / jnp.maximum(total_small[0:8, :], SCALE_FLOOR)
    for k in range(nc):
        scales[k] = ascale[k : k + 1, :]
    hb[...] = total_small[8:16, :]
    ch[pl.ds(hrow, 8), pl.ds(hcol, LANES)] = total_small[8:16, :]
    pv[0:8, :] = apeak
    for k in range(wp // LANES):
        pv[8 + k : 9 + k, :] = gpeak[:, k * LANES : (k + 1) * LANES]
    pv[8 + wp // LANES :, :] = jnp.zeros((8 - wp // LANES, LANES), jnp.float32)
    p2_copy().start()

    def r1_copy(s):
        return rcopy(s1.at[s], r1.at[s], sr1, rr1.at[s], other_core)

    def r4_copy(s):
        return rcopy(s4.at[s], rb.at[zp], sr4, rr4, pair_dev(chunk(s)))

    def compute(s):
        scale = scales[chunk(s)]
        for i in range(nt):
            v = g[s * nt + i].astype(jnp.float32) * scale
            q[pl.ds(i * rows, rows), :] = jnp.clip(v, -QUANT_LIMIT, QUANT_LIMIT).astype(jnp.bfloat16)
        out = jnp.dot(gq[...], q[...], preferred_element_type=jnp.float32)
        part[...] = out.T.reshape(8, 16, wp)

    def start_r1(s):
        for i in range(4):
            s1[s, i] = part[2 * i + 1 - c].astype(jnp.bfloat16)
        r1_copy(s).start()

    def quad_copy(s, i):
        zz, yy, _ = cube_index(2 * i)
        return rcopy(
            s2.at[s * 3 + i - 1], r2.at[s * 3 + i - 1], sr2, rr2.at[s], dp_dev(2 * zp + zz, yy, c)
        )

    def finish_r1(s):
        r1_copy(s).wait_recv()
        for i in range(4):
            zz, yy, _ = cube_index(2 * i)
            k = 2 * zz + yy
            total = part[2 * k + c] + r1[s, k].astype(jnp.float32)
            if i == 0:
                keep2[s % 4] = total
            else:
                s2[s * 3 + i - 1] = total.astype(jnp.bfloat16)
        for i in range(1, 4):
            quad_copy(s, i).start()

    def finish_quad(s):
        total = keep2[s % 4]
        a = r2.at[pl.ds(s * 3, 3)]
        rcopy(a, a, sr2, rr2.at[s], other_core).wait_recv()
        for i in range(3):
            total = total + r2[s * 3 + i].astype(jnp.float32)
        emit(s, total)

    def emit(s, total):
        s4[s] = total.astype(jnp.bfloat16)

        @pl.when(chunk(s) == zp)
        def _():
            own_sum[...] = total

        @pl.when(chunk(s) != zp)
        def _():
            r4_copy(s).start()

    def p3_copy():
        return rcopy(pcore, pylo, sp3, rp3, other_yl)

    def p4_copy():
        return rcopy(pylo, pzz, sp4, rp4, other_z)

    def p5_copy(i):
        return rcopy(pzz, pfar.at[i], sp5, rp5, pair_dev((zp + i) % nc))

    def h3_copy(i):
        dst = ch.at[pl.ds(hrow, 8), pl.ds(hcol, LANES)]
        return rcopy(hb, dst, sh3, rh3, pair_dev((zp + i) % nc))

    def h3_all():
        a = ch.at[pl.ds(0, 8), pl.ds(0, (nc - 1) * LANES)]
        return rcopy(a, a, sh3, rh3, other_core)

    def p5_all():
        a = pfar.at[pl.ds(1, nc - 1)]
        return rcopy(a, a, sp5, rp5, other_core)

    def h4_copy():
        half = ch.at[pl.ds(hrow, 8), :]
        return rcopy(half, half, sh4, rh4, other_core)

    def h4_arrival():
        half = ch.at[pl.ds(pl.multiple_of(8 - hrow, 8), 8), :]
        return rcopy(half, half, sh4, rh4, other_core)

    def side_work(s):
        def p3():
            p2_copy().wait_recv()
            pcore[...] = jnp.maximum(pcore[...], pv[...])
            p3_copy().start()

        def p4():
            p3_copy().wait_recv()
            pylo[...] = jnp.maximum(pylo[...], pcore[...])
            p4_copy().start()

        def far():
            p4_copy().wait_recv()
            pzz[...] = jnp.maximum(pzz[...], pylo[...])
            for i in range(1, nc):
                h3_copy(i).start()
            for i in range(1, nc):
                p5_copy(i).start()

        todo = [(0, p3), (1, p4), (2, far)]
        for at, work in todo:
            pl.when(s == min(at, nc - 1))(work)

    def tokens_wait():
        @pl.when(zp < early)
        def _():
            pl.semaphore_wait(tok1, nc - 1 - zp)
            for pp in range(early, nc):
                @pl.when((nc - 1 - pp) % early == zp)
                def _():
                    signal(tok2, pair_dev(pp))

        @pl.when(zp >= early)
        def _():
            pl.semaphore_wait(tok2, 1)

    def step(s, carry):
        @pl.when(s + AHEAD + 1 < nc)
        def _():
            start_y(s + AHEAD + 1)

        @pl.when(s + AHEAD < nc)
        def _():
            stage_own(s + AHEAD)

        @pl.when(s >= 1)
        def _():
            finish_r1(s - 1)

        stage_finish(s)
        compute(s)
        start_r1(s)

        @pl.when(jnp.logical_and(s == 0, AHEAD - 3 < nc))
        def _():
            stage_far_other(s + AHEAD - 3)

        @pl.when(s + AHEAD - 1 < nc)
        def _():
            stage_partner(s + AHEAD - 1)
            stage_far_own(s + AHEAD - 1)

        @pl.when(s == tok_step)
        def _():
            tokens_wait()

        @pl.when(jnp.logical_and(s >= 2, jnp.logical_or(s < nc - 1, zp > 0)))
        def _():
            finish_quad(s - 2)

        @pl.when(s + AHEAD - 2 < nc)
        def _():
            stage_far_other(s + AHEAD - 2)

        side_work(s)
        return carry

    lax.fori_loop(0, nc, step, 0)
    last = nc - 1
    finish_r1(last)
    if nc > 2:
        @pl.when(zp == 0)
        def _():
            finish_quad(last - 2)

    h3_all().wait_recv()
    h4_copy().start()
    if nc > 1:
        finish_quad(last - 1)
    top = pzz[...]
    p5_all().wait_recv()
    for i in range(1, nc):
        top = jnp.maximum(top, pfar[i])
    for k in range(nc):
        peak_row[:, k * LANES : (k + 1) * LANES] = top[k : k + 1, :]
    for k in range(wp // LANES):
        n = min(width - k * LANES, LANES)
        gpeak_row[:, k * LANES : k * LANES + n] = top[8 + k : 9 + k, :n]
    hist_row = lax.broadcasted_iota(jnp.int32, (16, width), 0)
    pack_out[16:32, :] = jnp.where(hist_row == gsl[...], gpeak_row[...], gh[...])
    h4_arrival().wait_recv()
    hist_row = lax.broadcasted_iota(jnp.int32, hist_out.shape, 0)
    hist_out[...] = jnp.where(hist_row == sl[:, : nc * LANES], peak_row[...], ch[...])
    lane = lax.broadcasted_iota(jnp.int32, (16, LANES), 1)
    row = lax.broadcasted_iota(jnp.int32, (16, LANES), 0)
    mine = lane == row + (zq * 4 + yl * 2 + c) * 16
    row_scale = jnp.sum(jnp.where(mine, scales[zp], jnp.float32(0.0)), axis=1, keepdims=True)
    gscale = QUANT_LIMIT / jnp.maximum(jnp.max(gh[...], axis=0, keepdims=True), SCALE_FLOOR)
    finish_quad(last)

    total = own_sum[...]
    a = rb.at[pl.ds(0, nc - 1)]
    rcopy(a, a, sr4, rr4, other_core).wait_recv()
    for i in range(1, nc):
        frm = (zp + i) % nc
        total = total + rb[frm].astype(jnp.float32)
    pack_out[0:16, :] = total[:, :width] / (row_scale * gscale)

    for a, done in (
        (g.at[pl.ds(0, 7 * nc)], sg.at[0]),
        (small.at[pl.ds(0, 7)], sg.at[1]),
        (s1, sr1),
        (s2, sr2),
        (s4.at[pl.ds(0, nc - 1)], sr4),
    ):
        rcopy(a, a, done, rr4, other_core).wait_send()
    h4_copy().wait_send()
    p2_copy().wait_send()
    p3_copy().wait_send()
    p4_copy().wait_send()
    h3_all().wait_send()
    p5_all().wait_send()


def fused(acts, grads, ahist, ghist, owner, slots, nz, nx):
    rows, model = acts.shape
    width, tokens = grads.shape
    nc, nt = nz // 2, 2 * nx
    wp = -(-width // LANES) * LANES
    f32, bf16 = jnp.float32, jnp.bfloat16
    dma = pltpu.SemaphoreType.DMA
    vm = pltpu.VMEM
    scratch = [
        vm((nc * nt, rows, LANES), bf16),
        vm((rows, model), bf16),
        vm((width, tokens), bf16),
        vm((wp, tokens), bf16),
        vm((tokens, LANES), bf16),
        vm((1, 16, model), f32),
        vm((16, width), f32),
        vm((1, model), jnp.int32),
        vm((1, slots.shape[0]), jnp.int32),
        vm((1, width), jnp.int32),
        vm((1, model), f32),
        vm((1, width), f32),
        vm((wp, LANES), f32),
        vm((wp, LANES), f32),
        vm((nc, 1, LANES), f32),
        vm((16, model), f32),
        vm((nt, 24, LANES), f32),
        vm((8, LANES), f32),
        vm((16, model), f32),
        vm((16, LANES), f32),
        vm((16, LANES), f32),
        vm((16, LANES), f32),
        vm((16, LANES), f32),
        vm((nc, 16, LANES), f32),
        vm((8, 16, wp), f32),
        vm((nc, 4, 16, wp), bf16),
        vm((nc, 4, 16, wp), bf16),
        vm((nc * 3, 16, wp), bf16),
        vm((nc * 3, 16, wp), bf16),
        vm((4, 16, wp), f32),
        vm((nc, 16, wp), bf16),
        vm((nc, 16, wp), bf16),
        vm((16, wp), f32),
        dma((2,)), dma((6,)),
        dma((2,)), dma((nc + 1, 4)),
        dma, dma, dma, dma,
        dma, dma, dma, dma, dma, dma, dma, dma,
        dma, dma((nc,)), dma, dma((nc,)), dma, dma,
        pltpu.SemaphoreType.REGULAR, pltpu.SemaphoreType.REGULAR,
    ]
    vspec = pl.BlockSpec(memory_space=pltpu.VMEM)
    anyspec = pl.BlockSpec(memory_space=pl.ANY)
    return pl.pallas_call(
        functools.partial(kernel, nz, nx),
        out_shape=[
            jax.ShapeDtypeStruct((32, width), f32),
            jax.ShapeDtypeStruct((16, model), f32),
        ],
        in_specs=[anyspec] * 6,
        out_specs=[vspec] * 2,
        scratch_shapes=scratch,
        compiler_params=pltpu.CompilerParams(
            collective_id=0, has_side_effects=True, vmem_limit_bytes=60 * 1024 * 1024
        ),
    )(acts, grads, ahist, ghist, owner, slots)


def body(nz, nx, activations, gradients, act_history, grad_history, owner_rank, history_slot):
    factor = 1.0 / math.sqrt(gradients.shape[0] * lax.axis_size("dp"))
    packed, act_history_out = fused(
        activations, gradients.T, act_history, grad_history,
        owner_rank.reshape(1, -1), history_slot, nz, nx,
    )
    return (packed[:16] * factor, jnp.abs(act_history_out)[None], jnp.abs(packed[16:]))


def solution(mesh):
    nz = mesh.shape["dp"] // 4
    nx = mesh.shape["tensor"] // 2
    placed = (
        P(("dp", "tensor"), None),
        P("dp", "tensor"),
        P("tensor", None, None),
        P(None, "tensor"),
        P(),
        P(),
    )
    return jax.shard_map(
        functools.partial(body, nz, nx),
        mesh=mesh,
        in_specs=placed,
        out_specs=(P("dp", "tensor"), P("tensor", None, None), P(None, "tensor")),
        check_vma=False,
    )
```
